32 devices in a mesh: users: 16 (over z, y, x), cols: 2 (over core).
Axes of the slice: x: 2, y: 2, z: 4, core: 2. Of those that a mesh axis runs over, the one named last changes fastest.
Arguments:
- item_ids: int32 [256, 256], P('users'), may hold values from 0 to 32767, as said below
- lengths: int32 [256], P('users'), may hold values from 1 to 256, 40960 in all
- seed_rows: int32 [256, 256], P('users'), may hold values from 0 to 63
- item_table: bfloat16 [32768, 1024], P('users', 'cols'), may hold values from -0.59765625 to 0.59765625
- bilinear: bfloat16 [1024, 1024], P(None, 'cols'), may hold values from -0.1875 to 0.1875
- seed_table: float32 [64, 8], replicated, may hold values from -260 to 260
Outputs:
- capsules: float32 [256, 8, 1024], P('users', None, 'cols')
The draws below stay inside these ranges and needn't reach their ends.
Inputs may be any that keep to these rules, and one draw needn't show every extreme that they name: `item_ids`: ids 2048 * s to 2048 * (s + 1) - 1 form table shard s. Of the 4096 ids of one index of users, at most 512 lie in one shard, and exactly 512 lie in some shard.
All inputs are finite; a program needn't handle non-finite values. No bound on the sum of `lengths` on one device may be relied on, other than what follows from the above.
Results may differ from the reference program's by a relative error of at most 0.0046.
Values may be sent and summed in bfloat16 or wider, within the bound.
No kernel may reach another device: no remote copies, remote signals or barrier semaphores. Data moves between devices by JAX's collectives and lax.ppermute only.
A program may use at most 128 MiB of HBM per device.

```python
import math
import jax
import jax.numpy as jnp
import numpy as np
from jax import lax

D = 1024
K = 8
HIST = 256
ITERS = 3
SEEDS = 64
U_DEV = 16
ROWS_DEV = 2048
USERS = 256
VOCAB = 32768
CAP = 512


def draw_item_ids(key, part):
    blocks = USERS // U_DEV
    tok_count = U_DEV * HIST
    owners = VOCAB // ROWS_DEV

    def draw_block(block_index):
        block_key = jax.random.fold_in(key, block_index)
        key_perm, key_hot, key_mix, key_rows = jax.random.split(block_key, 4)
        shuffled = jax.random.permutation(key_perm, owners * CAP)
        hot_owner = jax.random.randint(key_hot, (), 0, owners)
        priority = jnp.where(shuffled // CAP == hot_owner, 0, 1).astype(jnp.int32)
        ranking = jnp.argsort(priority, stable=True)
        chosen = shuffled[ranking][:tok_count]
        chosen = chosen[jax.random.permutation(key_mix, tok_count)]
        row_in = jax.random.randint(key_rows, (tok_count,), 0, ROWS_DEV)
        return (chosen // CAP * ROWS_DEV + row_in).astype(jnp.int32)
    return jax.vmap(draw_block)(jnp.arange(blocks)).reshape(USERS, HIST)


def draw_seed_table(key, part):
    key_base = jax.random.fold_in(jax.random.fold_in(key, 7), 0)
    return 1.5 * jax.random.normal(key_base, (SEEDS, K), jnp.float32)


def set_ends(values, own_key, least, high):
    shape = values.shape
    place = [jax.random.randint(jax.random.fold_in(own_key, axis), (), 0, shape[axis]) for axis in range(len(shape))]
    values = values.at[tuple(place)].set(least)
    longest = shape.index(max(shape))
    place[longest] = (place[longest] + 1) % shape[longest]
    return values.at[tuple(place)].set(high)


def block_scale(rng, shape, cuts, smallest, top_value):
    def one(axis_at, shards_of):
        steps = jax.random.uniform(jax.random.fold_in(jax.random.fold_in(rng, 6), axis_at), (shards_of,), jnp.float32, smallest / len(cuts), top_value / len(cuts))
        return jnp.repeat(jnp.exp(steps), shape[axis_at] // shards_of).reshape((-1,) + (1,) * (len(shape) - axis_at - 1))

    loudness = one(*cuts[0])
    for cut in cuts[1:]:
        loudness = loudness * one(*cut)
    return loudness


def length_profile(count, total, limit, lean):
    portions = [(1 << 20) // math.isqrt(standing ** lean) + 1 for standing in range(2, count + 1)]
    rest, counts = total - limit - (count - 1), [1] * (count - 1)
    while rest > 0:
        movable = [i for i in range(count - 1) if counts[i] < limit]
        whole, budget = sum([portions[i] for i in movable]), rest
        for i in movable:
            addition = min(limit - counts[i], max(1, budget * portions[i] // whole), rest)
            counts[i] = counts[i] + addition
            rest = rest - addition
    return np.array([limit] + counts)


def ragged_sizes(rng, amount, total, bound, skew):
    if amount == 2:
        one = jax.random.randint(rng, (), max(1, total - bound), min(bound, total - 1) + 1)
        return jnp.stack([one, total - one])
    sizes = jnp.asarray(length_profile(amount, total, bound, skew), jnp.int32)
    pairs = (amount - 1) // 2
    source_of, receiver = sizes[1:1 + 2 * pairs:2], sizes[2:2 + 2 * pairs:2]
    margin = jnp.minimum(source_of - 1, bound - receiver)
    moved = jax.random.randint(jax.random.fold_in(rng, 1), (pairs,), 0, 1 << 20) % (margin + 1)
    sizes = sizes.at[1:1 + 2 * pairs:2].set(source_of - moved).at[2:2 + 2 * pairs:2].set(receiver + moved)
    return sizes[jax.random.permutation(jax.random.fold_in(rng, 2), amount)]


def normal_values(rng, dims, scale, limit, pieces=(), kind=jnp.bfloat16):
    values = jax.random.normal(rng, dims, jnp.float32) * scale
    if len(pieces) > 0:
        values = block_scale(rng, dims, pieces, -0.22, 0.18) * values
    return jnp.clip(values, min=-limit, max=limit).astype(kind)


def setup_inputs(seed: int = 0) -> dict:
    key_of = jax.random.split(jax.random.key(seed), 7)
    return {
        "item_ids": draw_item_ids(jax.random.fold_in(key_of[6], 71), 0),
        "lengths": ragged_sizes(key_of[1], USERS, USERS * HIST * 5 // 8, HIST, 2).astype(jnp.int32),
        "seed_rows": set_ends(jax.random.randint(key_of[2], (USERS, HIST), 0, SEEDS), jax.random.fold_in(key_of[2], 1), 0, SEEDS - 1).astype(jnp.int32),
        "item_table": normal_values(key_of[3], (VOCAB, D), 0.1, 0.59765625, ((0, 16), (1, 2))),
        "bilinear": normal_values(key_of[4], (D, D), D ** -0.5, 0.1875, ((1, 2),)),
        "seed_table": draw_seed_table(jax.random.fold_in(key_of[6], 71), 0),
    }


def squash_scale(squares):
    return squares / (1.0 + squares) / jnp.sqrt(squares + 1e-06)

def reference(item_ids, lengths, seed_rows, item_table, bilinear, seed_table):
    blocks = USERS // U_DEV

    def per_block(inputs):
        block_ids, block_seeds, block_lens = inputs
        embedded = item_table[block_ids.reshape(-1)]
        mapped = jnp.dot(embedded, bilinear, preferred_element_type=jnp.float32).astype(jnp.bfloat16)
        mapped = lax.optimization_barrier(mapped).astype(jnp.float32).reshape(U_DEV, HIST, D)
        logits = seed_table[block_seeds]
        position = jnp.arange(HIST, dtype=jnp.int32)
        live = (position[None, :] < block_lens[:, None]).astype(jnp.float32)
        capsules = jnp.zeros((U_DEV, K, D), jnp.float32)
        for step in range(ITERS):
            weights = (jax.nn.softmax(logits, axis=-1) * live[:, :, None]).astype(jnp.bfloat16)
            weights = lax.optimization_barrier(weights).astype(jnp.float32)
            summed = jnp.einsum('utk,utd->ukd', weights, mapped, precision=lax.Precision.HIGHEST)
            squares = lax.optimization_barrier(jnp.sum(summed * summed, axis=-1))
            capsules = summed * squash_scale(squares)[:, :, None]
            if step + 1 < ITERS:
                logits = logits + jnp.einsum('utd,ukd->utk', mapped, capsules, precision=lax.Precision.HIGHEST)
        return capsules
    result = lax.map(per_block, (item_ids.reshape(blocks, U_DEV, HIST), seed_rows.reshape(blocks, U_DEV, HIST), lengths.reshape(blocks, U_DEV)))
    return result.reshape(USERS, K, D)
```

```python
import functools

import jax
import jax.numpy as jnp
from jax import lax
from jax.experimental import pallas as pl
from jax.experimental.pallas import tpu as pltpu
from jax.sharding import PartitionSpec as P

ITERS = 3
F32, BF16, I32 = jnp.float32, jnp.bfloat16, jnp.int32
NT = (((1,), (1,)), ((), ()))
VMEM = pl.BlockSpec(memory_space=pltpu.VMEM)
SMEM = pl.BlockSpec(memory_space=pltpu.SMEM)


def squash_scale(squares):
    return squares / (1.0 + squares) / jnp.sqrt(squares + 1e-06)


def div_mod(value, by):
    if by & (by - 1) == 0:
        return value >> (by.bit_length() - 1), value & (by - 1)
    quotient = lax.div(value, jnp.full(value.shape, by, I32))
    return quotient, value - quotient * by


def iota(shape, dim):
    return lax.broadcasted_iota(I32, shape, dim)


def dot(a, b):
    return jnp.dot(a, b, preferred_element_type=F32)


def dot_nt(a, b, **kw):
    return lax.dot_general(a, b, NT, preferred_element_type=F32, **kw)


def bits(mask):
    return jnp.where(mask, 1.0, 0.0).astype(BF16)


def pick(mask, value):
    return jnp.where(mask, value.astype(F32), 0.0).astype(BF16)


def positions(owner, owners):
    users, hist = owner.shape
    masks = jnp.concatenate([jnp.where(owner == s, 1.0, 0.0) for s in range(owners)], axis=0).astype(BF16)
    before = bits(iota((hist, hist), 0) < iota((hist, hist), 1))
    within = dot(masks, before)
    totals = dot(masks, jnp.ones((hist, hist), BF16))
    stacked = owners * users
    si, ui = div_mod(iota((stacked, stacked), 0), users)
    sj, uj = div_mod(iota((stacked, stacked), 1), users)
    earlier = dot(bits((si == sj) & (uj < ui)), totals.astype(BF16))
    rank = within + earlier
    pos = jnp.full(owner.shape, -1.0, F32)
    for s in range(owners):
        pos = jnp.where(owner == s, rank[s * users : (s + 1) * users], pos)
    return pos.astype(I32), masks


def prep_kernel(local_ref, ids_ref, seeds_ref, col_ref, row_ref, blocks_ref, dest_ref, *, owners, rows_dev, seeds, cap):
    users, hist = ids_ref.shape
    col, row = col_ref[...], row_ref[...]
    i, j = iota((users, users), 1), iota((users, users), 0)
    ahead = (row > col) | ((row == col) & (i < j))
    rank = jnp.sum(jnp.where(ahead, 1.0, 0.0), axis=1, keepdims=True).astype(I32)
    dest = div_mod(rank + local_ref[0], users)[1]
    dest_ref[...] = dest
    live = iota((users, hist), 1) < col
    packed = jnp.where(live, ids_ref[...] * seeds + seeds_ref[...], -1)
    place = iota((users, hist), 0)
    meta = jnp.full((users, hist), -1, I32)
    for j in range(users):
        meta = jnp.where(place == dest[j : j + 1, :], packed[j : j + 1, :], meta)
    ids = div_mod(meta, seeds)[0]
    owner, row_in = div_mod(ids, rows_dev)
    owner = jnp.where(meta >= 0, owner, -1)
    pos, masks = positions(owner, owners)
    lists = jnp.zeros((owners, cap), F32)
    slot = iota((cap, hist), 0)
    shard = iota((owners, hist), 0)
    for v in range(users):
        onehot = bits(slot == pos[v : v + 1, :])
        mine = shard == owner[v : v + 1, :]
        value = row_in[v : v + 1, :] + v * rows_dev
        low = value & 255
        lists = lists + dot_nt(pick(mine, low), onehot) + dot_nt(pick(mine, value - low), onehot)
    counts = dot_nt(jnp.ones((8, hist), BF16), masks)
    pairs = owners * users
    blocks_ref[:, :cap] = lists.astype(I32)
    blocks_ref[:, cap : cap + pairs] = jnp.broadcast_to(counts[:1].astype(I32), (owners, pairs))
    for group in range(owners // users):
        blocks_ref[group * users : (group + 1) * users, cap + pairs :] = meta


def owner_kernel(me_ref, recv_ref, mapped_ref, send_ref, index_ref, *, users, cap):
    v = pl.program_id(0)
    room = send_ref.shape[1]
    rows_dev = mapped_ref.shape[0]
    pairs = recv_ref.shape[0] * users
    local = lax.rem(v, users)

    @pl.when(local == 0)
    def _():
        got = recv_ref[pl.ds(pl.multiple_of(v, users), users), :]
        lists, counts = got[:, :cap], got[:, cap : cap + pairs].astype(F32).astype(BF16)
        s, w = div_mod(iota((pairs, 128), 0), users)
        lane = iota((pairs, 128), 1)
        here = s == me_ref[0]
        count = dot(counts, bits(here & (w == lane)))
        start = dot(counts, bits(here & (w < lane)))
        earlier = bits(iota((users, users), 1) < iota((users, users), 0))
        delta = (dot(earlier, count.astype(BF16)) - start).astype(I32)
        total = start[:, users : users + 1].astype(I32)
        rank = iota((users, cap), 1)
        valid = rank < total
        to, row = div_mod(lists, rows_dev)
        to = jnp.where(valid, to, -1)
        pos = rank
        for w in range(users):
            pos = pos + jnp.where(to == w, delta[:, w : w + 1], 0)
        pos = jnp.where(valid, pos, -1)
        slot = iota((room, cap), 0)
        shard = iota((users, cap), 0)
        index = jnp.zeros((room, users), F32)
        for u in range(users):
            onehot = bits(slot == pos[u : u + 1, :])
            mine = shard == to[u : u + 1, :]
            value = row[u : u + 1, :]
            low = value & 255
            index = index + dot_nt(onehot, pick(mine, low)) + dot_nt(onehot, pick(mine, value - low))
        index_ref[...] = index

    column = jnp.sum(jnp.where(iota(index_ref.shape, 1) == local, index_ref[...], 0.0), axis=1, keepdims=True)
    onehot = bits(iota((room, rows_dev), 1) == column.astype(I32))
    send_ref[0] = dot(onehot, mapped_ref[...]).astype(BF16)


def meta_kernel(meta_ref, seed_ref, user_ref, *, owners, rows_dev, seeds):
    users, hist = meta_ref.shape
    room = seed_ref.shape[1]
    meta = meta_ref[...]
    ids, seed = div_mod(meta, seeds)
    owner = jnp.where(meta >= 0, div_mod(ids, rows_dev)[0], -1)
    pos, _ = positions(owner, owners)
    slot = iota((room, hist), 0)
    shard = iota((owners, hist), 0)
    found = jnp.zeros((2 * owners, room), F32)
    for u in range(users):
        onehot = bits(slot == pos[u : u + 1, :])
        mine = shard == owner[u : u + 1, :]
        both = jnp.concatenate([jnp.where(mine, seed[u : u + 1, :].astype(F32), 0.0), jnp.where(mine, u + 1.0, 0.0)], axis=0)
        found = found + dot_nt(both.astype(BF16), onehot)
    seed_ref[...] = found[:owners].astype(I32)
    user_ref[...] = found[owners:].astype(I32)


def route(logits_of, rows_ref, user_ref, summed_ref, logits_ref):
    owners, room, half = rows_ref.shape
    lanes = summed_ref.shape[0]
    for s in range(owners):
        logits = logits_of(s)
        if logits_ref is not None:
            logits_ref[s] = logits
        caps = logits.shape[0]
        user = user_ref[s : s + 1, :]
        top = jnp.max(logits, axis=0, keepdims=True)
        raised = jnp.exp(logits - top)
        weights = raised / jnp.sum(raised, axis=0, keepdims=True)
        spread = jnp.concatenate([jnp.where(user == u + 1, weights, 0.0) for u in range(lanes // caps)], axis=0)
        part = dot(spread.astype(BF16), rows_ref[s])
        if s == 0:
            summed_ref[...] = part
        else:
            summed_ref[...] += part


def chosen(values, user, caps):
    total = jnp.zeros((caps, user.shape[1]), F32)
    for u in range(values.shape[0] // caps):
        total = jnp.where(user == u + 1, values[u * caps : (u + 1) * caps], total)
    return total


def products(rows_ref, user_ref, summed_ref, sent_ref, caps):
    owners, room, half = rows_ref.shape
    summed = summed_ref[...]
    lanes = summed.shape[0]
    high = summed.astype(BF16)
    low = (summed - high.astype(F32)).astype(BF16)
    both = jnp.concatenate([high, low], axis=0)
    for s in range(owners):
        dots = dot_nt(both, rows_ref[s])
        dots = dots[:lanes] + dots[lanes:]
        sent_ref[s * caps : (s + 1) * caps, :room] = chosen(dots, user_ref[s : s + 1, :], caps)
    sent_ref[:lanes, room:] = jnp.broadcast_to(
        jnp.sum(summed * summed, axis=1, keepdims=True), (lanes, sent_ref.shape[1] - room)
    )
    if sent_ref.shape[0] > lanes:
        sent_ref[lanes:, room:] = jnp.zeros((sent_ref.shape[0] - lanes, sent_ref.shape[1] - room), F32)


def first_kernel(rows_ref, seed_ref, user_ref, table_ref, logits_ref, sent_ref, summed_ref):
    caps, seeds = table_ref.shape
    room = rows_ref.shape[1]

    def initial(s):
        onehot = jnp.where(iota((seeds, room), 0) == seed_ref[s : s + 1, :], 1.0, 0.0)
        return jnp.dot(table_ref[...], onehot, precision=lax.Precision.HIGHEST, preferred_element_type=F32)

    route(initial, rows_ref, user_ref, summed_ref, logits_ref)
    products(rows_ref, user_ref, summed_ref, sent_ref, caps)


def later_kernel(*refs, cols, last, lanes):
    parts, (rows_ref, user_ref, old_ref), outs = refs[:cols], refs[cols : cols + 3], refs[cols + 3 :]
    owners, room, half = rows_ref.shape
    caps = old_ref.shape[1]
    squares = sum(part[:lanes, room : room + 1] for part in parts)
    scale = squash_scale(squares)

    def updated(s):
        dots = sum(part[s * caps : (s + 1) * caps, :room] for part in parts)
        user = user_ref[s : s + 1, :]
        wide = jnp.broadcast_to(scale, (lanes, room))
        return old_ref[s] + dots * chosen(wide, user, caps)

    if last:
        summed_ref, square_ref = outs
        route(updated, rows_ref, user_ref, summed_ref, None)
        summed = summed_ref[...]
        square_ref[...] = jnp.broadcast_to(jnp.sum(summed * summed, axis=1, keepdims=True), square_ref.shape)
    else:
        logits_ref, sent_ref, summed_ref = outs
        route(updated, rows_ref, user_ref, summed_ref, logits_ref)
        products(rows_ref, user_ref, summed_ref, sent_ref, caps)


def call(kernel, out_shape, n_in, smem=(), **kw):
    ins = [SMEM if i in smem else VMEM for i in range(n_in)]
    return pl.pallas_call(kernel, out_shape=out_shape, in_specs=ins, out_specs=jax.tree.map(lambda _: VMEM, out_shape), **kw)


def shifted(x, by):
    cols = lax.axis_size("cols")
    return lax.ppermute(x, "cols", [((i + by) % cols, i) for i in range(cols)])


def all_cols(x):
    return [x] + [shifted(x, by) for by in range(1, lax.axis_size("cols"))]


def map_table(item_table, bilinear):
    cols = lax.axis_size("cols")
    mine = lax.axis_index("cols")
    width = item_table.shape[1]
    total = None
    for by, part in enumerate(all_cols(item_table)):
        at = lax.rem(mine + by, cols) * width
        factor = lax.dynamic_slice_in_dim(bilinear, at, width, 0)
        term = dot(part, factor)
        total = term if total is None else total + term
    return total.astype(BF16)


def owner_ranks(owner, owners):
    tok_count = owner.shape[0]
    span = min(256, tok_count)
    onehot = (owner[:, None] == jnp.arange(owners, dtype=I32)[None, :]).astype(F32)
    blocked = onehot.reshape(tok_count // span, span, owners)
    lower = (iota((span, span), 0) >= iota((span, span), 1)).astype(F32)
    within = jnp.einsum("ij,bjo->bio", lower, blocked)
    totals = within[:, -1, :]
    before = jnp.cumsum(totals, axis=0) - totals
    counts = (within + before[:, None, :]).reshape(tok_count, owners)
    return (jnp.sum(counts * onehot, axis=1) - 1.0).astype(I32)


def any_input(item_ids, lengths, seed_rows, mapped_rows, seed_table, cap):
    users_here, hist = item_ids.shape
    owners = lax.axis_size("users")
    rows_dev, half = mapped_rows.shape
    tok_count = users_here * hist
    flat_ids = item_ids.reshape(tok_count)
    owner = flat_ids // rows_dev
    slot = owner * cap + owner_ranks(owner, owners)
    requests = jnp.zeros((owners * cap,), I32).at[slot].set(flat_ids % rows_dev).reshape(owners, cap)
    asked = lax.all_to_all(requests, "users", split_axis=0, concat_axis=0, tiled=True)
    answers = lax.all_to_all(mapped_rows[asked], "users", split_axis=0, concat_axis=0, tiled=True)
    mapped = answers.reshape(owners * cap, half)[slot].reshape(users_here, hist, half)
    logits = seed_table[seed_rows]
    live = (jnp.arange(hist, dtype=I32)[None, :] < lengths[:, None]).astype(F32)
    for step in range(ITERS):
        weights = (jax.nn.softmax(logits, axis=-1) * live[:, :, None]).astype(BF16)
        summed = jnp.einsum("utk,utd->ukd", weights, mapped, preferred_element_type=F32)
        squares = sum(all_cols(jnp.sum(summed * summed, axis=-1)))
        scale = squash_scale(squares)
        if step + 1 < ITERS:
            dots = jnp.einsum(
                "utd,ukd->utk", mapped, summed, preferred_element_type=F32, precision=lax.Precision.HIGHEST
            )
            logits = logits + sum(all_cols(dots)) * scale[:, None, :]
    return summed * scale[:, :, None]


def on_device(item_ids, lengths, seed_rows, item_table, bilinear, seed_table):
    users, hist = item_ids.shape
    owners = lax.axis_size("users")
    cols = lax.axis_size("cols")
    me = lax.axis_index("users")
    rows_dev = item_table.shape[0]
    half = bilinear.shape[1]
    seeds, caps = seed_table.shape
    tok_count = users * hist
    cap = max(2, (2 * tok_count + owners - 1) // owners)
    room = -(-cap * 7 // 16 // 16) * 16
    pairs = owners * users
    lanes = users * caps
    assert owners % users == 0 and hist <= 256 and seeds <= 256 and rows_dev * users <= 65536
    local = lax.rem(me, users)
    group = me - local

    mapped_rows = map_table(item_table, bilinear)
    blocks, dest = call(
        functools.partial(prep_kernel, owners=owners, rows_dev=rows_dev, seeds=seeds, cap=cap),
        (jax.ShapeDtypeStruct((owners, cap + pairs + hist), I32), jax.ShapeDtypeStruct((users, 1), I32)),
        5,
        smem=(0,),
    )(local.reshape(1), item_ids, seed_rows, lengths.reshape(users, 1), lengths.reshape(1, users))
    recv = lax.all_to_all(blocks, "users", split_axis=0, concat_axis=0, tiled=True)
    counts = recv[:, cap : cap + pairs].reshape(owners // users, users, pairs)
    fits = jnp.max(jnp.sum(counts, axis=1)) <= room

    def dealt(recv, mapped_rows, dest, seed_table, *_):
        width = recv.shape[1]
        send = pl.pallas_call(
            functools.partial(owner_kernel, users=users, cap=cap),
            grid=(owners,),
            out_shape=jax.ShapeDtypeStruct((owners, room, half), BF16),
            in_specs=[
                SMEM,
                pl.BlockSpec((owners, width), lambda v: (0, 0)),
                pl.BlockSpec((rows_dev, half), lambda v: (0, 0)),
            ],
            out_specs=pl.BlockSpec((1, room, half), lambda v: (v, 0, 0)),
            scratch_shapes=[pltpu.VMEM((room, users), F32)],
        )(me.reshape(1), recv, mapped_rows)
        rows = lax.all_to_all(send, "users", split_axis=0, concat_axis=0, tiled=True)
        meta = lax.dynamic_slice(recv, (group, cap + pairs), (users, hist))
        where = jax.ShapeDtypeStruct((owners, room), I32)
        seed, user = call(
            functools.partial(meta_kernel, owners=owners, rows_dev=rows_dev, seeds=seeds), (where, where), 1
        )(meta)
        logits_shape = jax.ShapeDtypeStruct((owners, caps, room), F32)
        wide = (room // 128 + 1) * 128
        sent_shape = jax.ShapeDtypeStruct((owners * caps, wide), F32)
        summed_shape = jax.ShapeDtypeStruct((lanes, half), F32)
        square_shape = jax.ShapeDtypeStruct((lanes, 128), F32)
        step_shapes = (logits_shape, sent_shape, summed_shape)
        logits, sent, _ = call(first_kernel, step_shapes, 4)(rows, seed, user, seed_table.T)
        for _ in range(ITERS - 2):
            kernel = functools.partial(later_kernel, cols=cols, last=False, lanes=lanes)
            logits, sent, _ = call(kernel, step_shapes, cols + 3)(*all_cols(sent), rows, user, logits)
        kernel = functools.partial(later_kernel, cols=cols, last=True, lanes=lanes)
        summed, square = call(kernel, (summed_shape, square_shape), cols + 3)(*all_cols(sent), rows, user, logits)
        scale = squash_scale(sum(all_cols(square))[:, :1])
        capsules = (summed * scale).reshape(users, caps, half)
        if owners > users:
            spread = jnp.zeros((owners, caps, half), F32)
            capsules = lax.dynamic_update_slice_in_dim(spread, capsules, group, 0)
        back = lax.all_to_all(capsules, "users", split_axis=0, concat_axis=0, tiled=True)
        if owners > users:
            back = lax.dynamic_slice_in_dim(back, group, users, 0)
        return back[dest[:, 0]]

    def full(recv, mapped_rows, dest, seed_table, item_ids, lengths, seed_rows):
        return any_input(item_ids, lengths, seed_rows, mapped_rows, seed_table, cap)

    return lax.cond(fits, dealt, full, recv, mapped_rows, dest, seed_table, item_ids, lengths, seed_rows)


def solution(mesh):
    placed = (
        P("users", None),
        P("users"),
        P("users", None),
        P("users", "cols"),
        P(None, "cols"),
        P(),
    )
    return jax.shard_map(
        on_device, mesh=mesh, in_specs=placed, out_specs=P("users", None, "cols"), check_vma=False
    )
```

```python
import functools
import math

import jax
import jax.numpy as jnp
from jax import lax
from jax.experimental import pallas as pl
from jax.experimental.pallas import tpu as pltpu
from jax.sharding import PartitionSpec as P


ITERS = 3
F32, BF16, I32 = jnp.float32, jnp.bfloat16, jnp.int32
NT = (((1,), (1,)), ((), ()))
VMEM = pl.BlockSpec(memory_space=pltpu.VMEM)
SMEM = pl.BlockSpec(memory_space=pltpu.SMEM)


def squash_scale(squares):
    return squares / (1.0 + squares) / jnp.sqrt(squares + 1e-06)


def div_mod(value, by):
    if by & (by - 1) == 0:
        return value >> (by.bit_length() - 1), value & (by - 1)
    quotient = lax.div(value, jnp.full(value.shape, by, I32))
    return quotient, value - quotient * by


def iota(shape, dim):
    return lax.broadcasted_iota(I32, shape, dim)


def dot(a, b):
    return jnp.dot(a, b, preferred_element_type=F32)


def dot_nt(a, b, **kw):
    return lax.dot_general(a, b, NT, preferred_element_type=F32, **kw)


def bits(mask):
    return jnp.where(mask, 1.0, 0.0).astype(BF16)


def halves(mask, value):
    low = value & 255
    both = [jnp.where(mask, term.astype(F32), 0.0) for term in (low, value - low)]
    return jnp.concatenate(both, axis=0).astype(BF16)


def positions(owner, owners):
    users, hist = owner.shape
    masks = jnp.concatenate([jnp.where(owner == s, 1.0, 0.0) for s in range(owners)], axis=0).astype(BF16)
    before = bits(iota((hist, hist), 0) < iota((hist, hist), 1))
    within = dot(masks, before)
    totals = dot(masks, jnp.ones((hist, hist), BF16))
    stacked = owners * users
    si, ui = div_mod(iota((stacked, stacked), 0), users)
    sj, uj = div_mod(iota((stacked, stacked), 1), users)
    earlier = dot(bits((si == sj) & (uj < ui)), totals.astype(BF16))
    rank = within + earlier
    pos = jnp.full(owner.shape, -1.0, F32)
    for s in range(owners):
        pos = jnp.where(owner == s, rank[s * users : (s + 1) * users], pos)
    return pos.astype(I32), masks


def prep_kernel(local_ref, ids_ref, seeds_ref, row_ref, blocks_ref, dest_ref, *, owners, rows_dev, seeds, cap):
    users, hist = ids_ref.shape
    row = row_ref[...]
    i, j = iota((users, users), 1), iota((users, users), 0)
    col = jnp.sum(jnp.where(i == j, row.astype(F32), 0.0), axis=1, keepdims=True).astype(I32)
    ahead = (row > col) | ((row == col) & (i < j))
    rank = jnp.sum(jnp.where(ahead, 1.0, 0.0), axis=1, keepdims=True).astype(I32)
    dest = div_mod(rank + local_ref[0], users)[1]
    dest_ref[...] = dest
    live = iota((users, hist), 1) < col
    packed = jnp.where(live, ids_ref[...] * seeds + seeds_ref[...], -1)
    place = iota((users, hist), 0)
    meta = jnp.full((users, hist), -1, I32)
    for j in range(users):
        meta = jnp.where(place == dest[j : j + 1, :], packed[j : j + 1, :], meta)
    ids = div_mod(meta, seeds)[0]
    owner, row_in = div_mod(ids, rows_dev)
    owner = jnp.where(meta >= 0, owner, -1)
    pos, masks = positions(owner, owners)
    lists = jnp.zeros((2 * owners, cap), F32)
    slot = iota((cap, hist), 0)
    shard = iota((owners, hist), 0)
    for v in range(users):
        onehot = bits(slot == pos[v : v + 1, :])
        mine = shard == owner[v : v + 1, :]
        lists = lists + dot_nt(halves(mine, row_in[v : v + 1, :] + v * rows_dev), onehot)
    lists = lists[:owners] + lists[owners:]
    counts = dot_nt(jnp.ones((8, hist), BF16), masks)
    pairs = owners * users
    blocks_ref[:, 0, :cap] = lists.astype(I32)
    blocks_ref[:, 0, cap : cap + pairs] = jnp.broadcast_to(counts[:1].astype(I32), (owners, pairs))
    for group in range(owners // users):
        blocks_ref[group * users : (group + 1) * users, 0, cap + pairs :] = meta


def map_kernel(*refs, cols):
    at_ref, factor_ref, parts, (out_ref,) = refs[0], refs[1], refs[2 : 2 + cols], refs[2 + cols :]
    rows, width = parts[0].shape
    tall = min(256, rows)

    def one(i, carry):
        here = pl.ds(pl.multiple_of(i * tall, tall), tall)
        total = None
        for by, part in enumerate(parts):
            at = pl.multiple_of(lax.rem(at_ref[0] + by, cols) * width, width)
            term = dot(part[here, :], factor_ref[pl.ds(at, width), :])
            total = term if total is None else total + term
        out_ref[here, :] = total.astype(BF16)
        return carry

    lax.fori_loop(0, rows // tall, one, 0)


def gather_rows(index, mapped_ref, loc):
    column = jnp.sum(jnp.where(iota(index.shape, 1) == loc, index, 0.0), axis=1, keepdims=True)
    onehot = bits(iota((index.shape[0], mapped_ref.shape[0]), 1) == column.astype(I32))
    return dot(onehot, mapped_ref[...]).astype(BF16)


def index_of(me, got, owners, cap, room, rows_dev):
    users = got.shape[0]
    pairs = owners * users
    lists, counts = got[:, :cap], got[:, cap : cap + pairs].astype(F32).astype(BF16)
    s, w = div_mod(iota((pairs, 128), 0), users)
    lane = iota((pairs, 128), 1)
    here = s == me
    count = dot(counts, bits(here & (w == lane)))
    start = dot(counts, bits(here & (w < lane)))
    earlier = bits(iota((users, users), 1) < iota((users, users), 0))
    delta = (dot(earlier, count.astype(BF16)) - start).astype(I32)
    total = start[:, users : users + 1].astype(I32)
    rank = iota((users, cap), 1)
    valid = rank < total
    to, row = div_mod(lists, rows_dev)
    to = jnp.where(valid, to, -1)
    pos = rank
    for w in range(users):
        pos = pos + jnp.where(to == w, delta[:, w : w + 1], 0)
    pos = jnp.where(valid, pos, -1)
    slot = iota((room, cap), 0)
    shard = iota((users, cap), 0)
    index = jnp.zeros((room, 2 * users), F32)
    for u in range(users):
        onehot = bits(slot == pos[u : u + 1, :])
        mine = shard == to[u : u + 1, :]
        index = index + dot_nt(onehot, halves(mine, row[u : u + 1, :]))
    return index[:, :users] + index[:, users:]


def send_blocks(me, index_ref, mapped_ref, outs, block_ref, first):
    users = index_ref.shape[2]

    def one(i, carry):
        group, loc = div_mod(me ^ (first + i), users)
        block_ref[...] = gather_rows(index_ref[group], mapped_ref, loc)
        for k, out_ref in enumerate(outs):
            @pl.when(i == k)
            def _(out_ref=out_ref):
                out_ref[...] = block_ref[...]
        return carry

    lax.fori_loop(0, len(outs), one, 0)


def index_kernel(me_ref, recv_ref, mapped_ref, index_ref, *refs, first, cap):
    groups, room, users = index_ref.shape
    for g in range(groups):
        got = recv_ref[g * users : (g + 1) * users, 0, :]
        index_ref[g] = index_of(me_ref[0], got, recv_ref.shape[0], cap, room, mapped_ref.shape[0])
    send_blocks(me_ref[0], index_ref, mapped_ref, refs[:-1], refs[-1], first)


def gather_kernel(me_ref, index_ref, mapped_ref, after_ref, order_ref, *refs, first):
    send_blocks(me_ref[0], index_ref, mapped_ref, refs[:-1], refs[-1], first)
    order_ref[...] = jnp.zeros(order_ref.shape, F32)


def meta_kernel(me_ref, recv_ref, seed_ref, user_ref, *, users, hist, rows_dev, seeds):
    owners, room = seed_ref.shape
    group = pl.multiple_of(div_mod(me_ref[0], users)[0] * users, users)
    meta = recv_ref[pl.ds(group, users), 0, recv_ref.shape[2] - hist :]
    ids, seed = div_mod(meta, seeds)
    owner = jnp.where(meta >= 0, div_mod(ids, rows_dev)[0] ^ me_ref[0], -1)
    pos, _ = positions(owner, owners)
    slot = iota((room, hist), 0)
    shard = iota((owners, hist), 0)
    found = jnp.zeros((2 * owners, room), F32)
    for u in range(users):
        onehot = bits(slot == pos[u : u + 1, :])
        mine = shard == owner[u : u + 1, :]
        both = jnp.concatenate([jnp.where(mine, seed[u : u + 1, :].astype(F32), 0.0), jnp.where(mine, u + 1.0, 0.0)], axis=0)
        found = found + dot_nt(both.astype(BF16), onehot)
    seed_ref[...] = found[:owners].astype(I32)
    user_ref[...] = found[owners:].astype(I32)


def route(logits_of, rows_refs, user_ref, summed_ref, logits_ref):
    owners = len(rows_refs)
    lanes = summed_ref.shape[0]
    for s in range(owners):
        logits = logits_of(s)
        if logits_ref is not None:
            logits_ref[s] = logits
        caps = logits.shape[0]
        user = user_ref[s : s + 1, :]
        top = jnp.max(logits, axis=0, keepdims=True)
        raised = jnp.exp(logits - top)
        weights = raised / jnp.sum(raised, axis=0, keepdims=True)
        spread = jnp.concatenate([jnp.where(user == u + 1, weights, 0.0) for u in range(lanes // caps)], axis=0)
        part = dot(spread.astype(BF16), rows_refs[s][...])
        if s == 0:
            summed_ref[...] = part
        else:
            summed_ref[...] += part


def chosen(values, user, caps):
    total = jnp.zeros((caps, user.shape[1]), F32)
    for u in range(values.shape[0] // caps):
        total = jnp.where(user == u + 1, values[u * caps : (u + 1) * caps], total)
    return total


def products(rows_refs, user_ref, summed_ref, sent_ref, caps):
    owners, room = len(rows_refs), rows_refs[0].shape[0]
    summed = summed_ref[...]
    lanes = summed.shape[0]
    high = summed.astype(BF16)
    low = (summed - high.astype(F32)).astype(BF16)
    both = jnp.concatenate([high, low], axis=0)
    for s in range(owners):
        dots = dot_nt(both, rows_refs[s][...])
        dots = dots[:lanes] + dots[lanes:]
        sent_ref[s * caps : (s + 1) * caps, :room] = chosen(dots, user_ref[s : s + 1, :], caps)
    sent_ref[:lanes, room:] = jnp.broadcast_to(
        jnp.sum(summed * summed, axis=1, keepdims=True), (lanes, sent_ref.shape[1] - room)
    )
    if sent_ref.shape[0] > lanes:
        sent_ref[lanes:, room:] = jnp.zeros((sent_ref.shape[0] - lanes, sent_ref.shape[1] - room), F32)


def first_kernel(*refs, owners):
    rows_refs, (seed_ref, user_ref, table_ref, logits_ref, sent_ref, summed_ref) = refs[:owners], refs[owners:]
    caps, seeds = table_ref.shape
    room = rows_refs[0].shape[0]

    def initial(s):
        onehot = jnp.where(iota((seeds, room), 0) == seed_ref[s : s + 1, :], 1.0, 0.0)
        return jnp.dot(table_ref[...], onehot, precision=lax.Precision.HIGHEST, preferred_element_type=F32)

    route(initial, rows_refs, user_ref, summed_ref, logits_ref)
    products(rows_refs, user_ref, summed_ref, sent_ref, caps)


def later_kernel(*refs, cols, last, owners, lanes):
    parts, rows_refs, refs = refs[:cols], refs[cols : cols + owners], refs[cols + owners :]
    (user_ref, old_ref), outs = refs[:2], refs[2:]
    room = rows_refs[0].shape[0]
    caps = old_ref.shape[1]
    squares = sum(part[:lanes, room : room + 1] for part in parts)
    scale = squash_scale(squares)

    def updated(s):
        dots = sum(part[s * caps : (s + 1) * caps, :room] for part in parts)
        user = user_ref[s : s + 1, :]
        wide = jnp.broadcast_to(scale, (lanes, room))
        return old_ref[s] + dots * chosen(wide, user, caps)

    if last:
        summed_ref, square_ref = outs
        route(updated, rows_refs, user_ref, summed_ref, None)
        summed = summed_ref[...]
        square_ref[...] = jnp.broadcast_to(jnp.sum(summed * summed, axis=1, keepdims=True), square_ref.shape)
    else:
        logits_ref, sent_ref, summed_ref = outs
        route(updated, rows_refs, user_ref, summed_ref, logits_ref)
        products(rows_refs, user_ref, summed_ref, sent_ref, caps)


def squash_kernel(summed_ref, *refs):
    scale = squash_scale(sum(part[:, :1] for part in refs[:-1]))
    refs[-1][...] = summed_ref[...] * scale


def call(kernel, out_shape, n_in, smem=(), flops=0, mib=16, **kw):
    ins = [SMEM if i in smem else VMEM for i in range(n_in)]
    size = sum(math.prod(leaf.shape) * leaf.dtype.itemsize for leaf in jax.tree.leaves(out_shape))
    return pl.pallas_call(
        kernel,
        out_shape=out_shape,
        in_specs=ins,
        out_specs=jax.tree.map(lambda _: VMEM, out_shape),
        compiler_params=pltpu.CompilerParams(vmem_limit_bytes=mib << 20),
        cost_estimate=pl.CostEstimate(flops=flops, bytes_accessed=size, transcendentals=0),
        **kw,
    )


def shifted(x, by):
    cols = lax.axis_size("cols")
    return lax.ppermute(x, "cols", [((i + by) % cols, i) for i in range(cols)])


def all_cols(x):
    return [x] + [shifted(x, by) for by in range(1, lax.axis_size("cols"))]


def owner_ranks(owner, owners):
    tok_count = owner.shape[0]
    span = min(256, tok_count)
    onehot = (owner[:, None] == jnp.arange(owners, dtype=I32)[None, :]).astype(F32)
    blocked = onehot.reshape(tok_count // span, span, owners)
    lower = (iota((span, span), 0) >= iota((span, span), 1)).astype(F32)
    within = jnp.einsum("ij,bjo->bio", lower, blocked)
    totals = within[:, -1, :]
    before = jnp.cumsum(totals, axis=0) - totals
    counts = (within + before[:, None, :]).reshape(tok_count, owners)
    return (jnp.sum(counts * onehot, axis=1) - 1.0).astype(I32)


def any_input(item_ids, lengths, seed_rows, mapped_rows, seed_table, cap):
    users_here, hist = item_ids.shape
    owners = lax.axis_size("users")
    rows_dev, half = mapped_rows.shape
    tok_count = users_here * hist
    flat_ids = item_ids.reshape(tok_count)
    owner = flat_ids // rows_dev
    slot = owner * cap + owner_ranks(owner, owners)
    requests = jnp.zeros((owners * cap,), I32).at[slot].set(flat_ids % rows_dev).reshape(owners, cap)
    asked = lax.all_to_all(requests, "users", split_axis=0, concat_axis=0, tiled=True)
    answers = lax.all_to_all(mapped_rows[asked], "users", split_axis=0, concat_axis=0, tiled=True)
    mapped = answers.reshape(owners * cap, half)[slot].reshape(users_here, hist, half)
    logits = seed_table[seed_rows]
    live = (jnp.arange(hist, dtype=I32)[None, :] < lengths[:, None]).astype(F32)
    for step in range(ITERS):
        weights = (jax.nn.softmax(logits, axis=-1) * live[:, :, None]).astype(BF16)
        summed = jnp.einsum("utk,utd->ukd", weights, mapped, preferred_element_type=F32)
        squares = sum(all_cols(jnp.sum(summed * summed, axis=-1)))
        scale = squash_scale(squares)
        if step + 1 < ITERS:
            dots = jnp.einsum(
                "utd,ukd->utk", mapped, summed, preferred_element_type=F32, precision=lax.Precision.HIGHEST
            )
            logits = logits + sum(all_cols(dots)) * scale[:, None, :]
    return summed * scale[:, :, None]


def cuts_of(owners):
    far = owners // 2
    return [(far, far + 1), (far + 1, far + 4), (far + 4, owners), (0, far)]


def on_device(item_ids, lengths, seed_rows, item_table, bilinear, seed_table):
    users, hist = item_ids.shape
    owners = lax.axis_size("users")
    cols = lax.axis_size("cols")
    me = lax.axis_index("users")
    rows_dev = item_table.shape[0]
    half = bilinear.shape[1]
    seeds, caps = seed_table.shape
    tok_count = users * hist
    cap = max(2, (2 * tok_count + owners - 1) // owners)
    room = -(-cap * 15 // 32 // 16) * 16
    pairs = owners * users
    lanes = users * caps
    assert owners % users == 0 and owners & (owners - 1) == 0
    assert hist <= 256 and seeds <= 256 and rows_dev * users <= 65536
    local = lax.rem(me, users)
    group = me - local
    here = me.reshape(1)

    table_parts = all_cols(item_table)
    blocks, dest = call(
        functools.partial(prep_kernel, owners=owners, rows_dev=rows_dev, seeds=seeds, cap=cap),
        (jax.ShapeDtypeStruct((owners, 1, cap + pairs + hist), I32), jax.ShapeDtypeStruct((users, 1), I32)),
        4,
        smem=(0,),
    )(local.reshape(1), item_ids, seed_rows, lengths.reshape(1, users))
    recv = lax.all_to_all(blocks, "users", split_axis=0, concat_axis=0, tiled=True)
    mapped_rows = call(
        functools.partial(map_kernel, cols=cols),
        jax.ShapeDtypeStruct((rows_dev, half), BF16),
        2 + cols,
        smem=(0,),
        flops=2 * rows_dev * half * bilinear.shape[0],
    )(lax.axis_index("cols").reshape(1), bilinear, *table_parts)
    counts = recv[:, 0, cap : cap + pairs].reshape(owners // users, users, pairs)
    fits = jnp.max(jnp.sum(counts, axis=1)) <= room

    block = jax.ShapeDtypeStruct((room, half), BF16)
    scratch = [pltpu.VMEM((room, half), BF16)]
    each = 2 * room * half * rows_dev
    rows = [None] * owners
    cuts = cuts_of(owners)
    index = order = None
    for first, stop in cuts:
        many = stop - first
        if index is None:
            index, *sends = call(
                functools.partial(index_kernel, first=first, cap=cap),
                [jax.ShapeDtypeStruct((owners // users, room, users), F32)] + [block] * many,
                3,
                smem=(0,),
                flops=many * each,
                scratch_shapes=scratch,
            )(here, recv, mapped_rows)
            order = index
        else:
            order, *sends = call(
                functools.partial(gather_kernel, first=first),
                [jax.ShapeDtypeStruct((8, 128), F32)] + [block] * many,
                4,
                smem=(0,),
                flops=many * each,
                scratch_shapes=scratch,
            )(here, index, mapped_rows, order)
        for mask, out in zip(range(first, stop), sends):
            rows[mask] = out if mask == 0 else lax.ppermute(out, "users", [(i, i ^ mask) for i in range(owners)])

    where = jax.ShapeDtypeStruct((owners, room), I32)
    seed, user = call(
        functools.partial(meta_kernel, users=users, hist=hist, rows_dev=rows_dev, seeds=seeds), (where, where), 2, smem=(0,)
    )(here, recv)
    logits_shape = jax.ShapeDtypeStruct((owners, caps, room), F32)
    wide = (room // 128 + 1) * 128
    sent_shape = jax.ShapeDtypeStruct((owners * caps, wide), F32)
    summed_shape = jax.ShapeDtypeStruct((lanes, half), F32)
    square_shape = jax.ShapeDtypeStruct((lanes, 128), F32)
    step_shapes = (logits_shape, sent_shape, summed_shape)
    kernel = functools.partial(first_kernel, owners=owners)
    logits, sent, _ = call(kernel, step_shapes, owners + 3)(*rows, seed, user, seed_table.T)
    later = functools.partial(later_kernel, cols=cols, owners=owners, lanes=lanes)
    for _ in range(ITERS - 2):
        kernel = functools.partial(later, last=False)
        logits, sent, _ = call(kernel, step_shapes, cols + owners + 2)(*all_cols(sent), *rows, user, logits)
    kernel = functools.partial(later, last=True)
    summed, square = call(kernel, (summed_shape, square_shape), cols + owners + 2)(*all_cols(sent), *rows, user, logits)
    capsules = call(squash_kernel, summed_shape, cols + 1)(summed, *all_cols(square)).reshape(users, caps, half)
    if owners > users:
        spread = jnp.zeros((owners, caps, half), F32)
        capsules = lax.dynamic_update_slice_in_dim(spread, capsules, group, 0)
    back = lax.all_to_all(capsules, "users", split_axis=0, concat_axis=0, tiled=True)
    if owners > users:
        back = lax.dynamic_slice_in_dim(back, group, users, 0)
    dealt = back[dest[:, 0]]

    def kept(dealt, *_):
        return dealt

    def full(dealt, mapped_rows, seed_table, item_ids, lengths, seed_rows):
        return any_input(item_ids, lengths, seed_rows, mapped_rows, seed_table, cap)

    return lax.cond(fits, kept, full, dealt, mapped_rows, seed_table, item_ids, lengths, seed_rows)


def solution(mesh):
    placed = (
        P("users", None),
        P("users"),
        P("users", None),
        P("users", "cols"),
        P(None, "cols"),
        P(),
    )

    return jax.shard_map(on_device, mesh=mesh, in_specs=placed, out_specs=P("users", None, "cols"), check_vma=False)
```

```python
import functools
import math

import jax
import jax.numpy as jnp
from jax import lax
from jax.experimental import pallas as pl
from jax.experimental.pallas import tpu as pltpu
from jax.sharding import PartitionSpec as P


ITERS = 3
PLANE = 4
RELAYS = ((1, 2), (2, 4), (0, 1))
F32, BF16, I32 = jnp.float32, jnp.bfloat16, jnp.int32
NT = (((1,), (1,)), ((), ()))
VMEM = pl.BlockSpec(memory_space=pltpu.VMEM)
SMEM = pl.BlockSpec(memory_space=pltpu.SMEM)
FAR = pl.BlockSpec(memory_space=pltpu.HBM)


def squash_scale(squares):
    return squares / (1.0 + squares) / jnp.sqrt(squares + 1e-06)


def div_mod(value, by):
    if by & (by - 1) == 0:
        return value >> (by.bit_length() - 1), value & (by - 1)
    quotient = lax.div(value, jnp.full(value.shape, by, I32))
    return quotient, value - quotient * by


def iota(shape, dim):
    return lax.broadcasted_iota(I32, shape, dim)


def dot(a, b):
    return jnp.dot(a, b, preferred_element_type=F32)


def dot_nt(a, b, **kw):
    return lax.dot_general(a, b, NT, preferred_element_type=F32, **kw)


def bits(mask):
    return jnp.where(mask, 1.0, 0.0).astype(BF16)


def halves(mask, value):
    low = value & 255
    both = [jnp.where(mask, term.astype(F32), 0.0) for term in (low, value - low)]
    return jnp.concatenate(both, axis=0).astype(BF16)


def positions(owner, owners):
    users, hist = owner.shape
    masks = jnp.concatenate([jnp.where(owner == s, 1.0, 0.0) for s in range(owners)], axis=0).astype(BF16)
    before = bits(iota((hist, hist), 0) < iota((hist, hist), 1))
    within = dot(masks, before)
    totals = dot(masks, jnp.ones((hist, hist), BF16))
    stacked = owners * users
    si, ui = div_mod(iota((stacked, stacked), 0), users)
    sj, uj = div_mod(iota((stacked, stacked), 1), users)
    earlier = dot(bits((si == sj) & (uj < ui)), totals.astype(BF16))
    rank = within + earlier
    pos = jnp.full(owner.shape, -1.0, F32)
    for s in range(owners):
        pos = jnp.where(owner == s, rank[s * users : (s + 1) * users], pos)
    return pos.astype(I32), masks


def prep_kernel(local_ref, ids_ref, seeds_ref, row_ref, blocks_ref, dest_ref, *, owners, rows_dev, seeds, cap):
    users, hist = ids_ref.shape
    row = row_ref[...]
    i, j = iota((users, users), 1), iota((users, users), 0)
    col = jnp.sum(jnp.where(i == j, row.astype(F32), 0.0), axis=1, keepdims=True).astype(I32)
    ahead = (row > col) | ((row == col) & (i < j))
    rank = jnp.sum(jnp.where(ahead, 1.0, 0.0), axis=1, keepdims=True).astype(I32)
    turn = div_mod(rank + local_ref[0], users)[1]
    high, low = div_mod(turn, users // PLANE)
    dest = low * PLANE + high
    dest_ref[...] = dest
    live = iota((users, hist), 1) < col
    packed = jnp.where(live, ids_ref[...] * seeds + seeds_ref[...], -1)
    place = iota((users, hist), 0)
    meta = jnp.full((users, hist), -1, I32)
    for j in range(users):
        meta = jnp.where(place == dest[j : j + 1, :], packed[j : j + 1, :], meta)
    ids = div_mod(meta, seeds)[0]
    owner, row_in = div_mod(ids, rows_dev)
    owner = jnp.where(meta >= 0, owner, -1)
    pos, masks = positions(owner, owners)
    lists = jnp.zeros((2 * owners, cap), F32)
    slot = iota((cap, hist), 0)
    shard = iota((owners, hist), 0)
    for v in range(users):
        onehot = bits(slot == pos[v : v + 1, :])
        mine = shard == owner[v : v + 1, :]
        lists = lists + dot_nt(halves(mine, row_in[v : v + 1, :] + v * rows_dev), onehot)
    lists = lists[:owners] + lists[owners:]
    counts = dot_nt(jnp.ones((8, hist), BF16), masks)
    pairs = owners * users
    blocks_ref[:, 0, :cap] = lists.astype(I32)
    blocks_ref[:, 0, cap : cap + pairs] = jnp.broadcast_to(counts[:1].astype(I32), (owners, pairs))
    for group in range(owners // users):
        blocks_ref[group * users : (group + 1) * users, 0, cap + pairs :] = meta


def map_kernel(*refs, cols):
    at_ref, factor_ref, own_ref, others = refs[0], refs[1], refs[2], refs[3 : 2 + cols]
    out_ref, factor, own, block, done = refs[2 + cols :]
    rows, width = own_ref.shape
    tall = own.shape[1]
    tiles = rows // tall

    def fetch(i):
        return pltpu.make_async_copy(own_ref.at[pl.ds(i * tall, tall)], own.at[i], done.at[i])

    def store(i):
        return pltpu.make_async_copy(block.at[i], out_ref.at[pl.ds(i * tall, tall)], done.at[tiles + i])

    whole = pltpu.make_async_copy(factor_ref, factor, done.at[2 * tiles])
    whole.start()
    for i in range(tiles):
        fetch(i).start()
    whole.wait()
    for i in range(tiles):
        fetch(i).wait()
        total = None
        for by in range(cols):
            part = own[i] if by == 0 else others[by - 1][i * tall : (i + 1) * tall, :]
            at = pl.multiple_of(lax.rem(at_ref[0] + by, cols) * width, width)
            term = dot(part, factor[pl.ds(at, width), :])
            total = term if total is None else total + term
        block[i] = total.astype(BF16)
        store(i).start()
    for i in range(tiles):
        store(i).wait()


def gather_rows(index, mapped_ref, loc):
    column = jnp.sum(jnp.where(iota(index.shape, 1) == loc, index, 0.0), axis=1, keepdims=True)
    onehot = bits(iota((index.shape[0], mapped_ref.shape[0]), 1) == column.astype(I32))
    return dot(onehot, mapped_ref[...]).astype(BF16)


def decode(me, got, owners, cap, rows_dev):
    users = got.shape[0]
    pairs = owners * users
    lists, counts = got[:, :cap], got[:, cap : cap + pairs].astype(F32).astype(BF16)
    s, w = div_mod(iota((pairs, 128), 0), users)
    lane = iota((pairs, 128), 1)
    here = s == me
    count = dot(counts, bits(here & (w == lane)))
    start = dot(counts, bits(here & (w < lane)))
    valid = iota((users, cap), 1) < start[:, users : users + 1].astype(I32)
    to, row = div_mod(lists, rows_dev)
    return jnp.where(valid, to, -1), row, count, start


def index_of(me, got, owners, cap, room, rows_dev):
    users = got.shape[0]
    to, row, count, start = decode(me, got, owners, cap, rows_dev)
    earlier = bits(iota((users, users), 1) < iota((users, users), 0))
    delta = (dot(earlier, count.astype(BF16)) - start).astype(I32)
    pos = iota((users, cap), 1)
    for w in range(users):
        pos = pos + jnp.where(to == w, delta[:, w : w + 1], 0)
    pos = jnp.where(to >= 0, pos, -1)
    slot = iota((room, cap), 0)
    shard = iota((users, cap), 0)
    index = jnp.zeros((room, 2 * users), F32)
    for u in range(users):
        onehot = bits(slot == pos[u : u + 1, :])
        mine = shard == to[u : u + 1, :]
        index = index + dot_nt(onehot, halves(mine, row[u : u + 1, :]))
    return index[:, :users] + index[:, users:]


def send_set(me, mask, ranks_ref, mapped_ref, out_ref):
    high = mapped_ref.shape[0] // 128
    many = out_ref.shape[0]
    tall = many // 4 if many % 64 == 0 else many
    plane = div_mod(me, PLANE)[0] ^ mask
    ranks = ranks_ref[pl.ds(pl.multiple_of(plane * high, high), high), :]

    def one(t, carry):
        slot = iota((tall, 128), 0) + t * tall
        onehot = [bits(slot == ranks[h : h + 1, :]) for h in range(high)]
        here = pl.ds(pl.multiple_of(t * tall, tall), tall)
        out_ref[here, :] = dot(jnp.concatenate(onehot, axis=1), mapped_ref[...]).astype(BF16)
        return carry

    lax.fori_loop(0, many // tall, one, 0)


def rank_kernel(me_ref, recv_ref, far_ref, ranks_ref, over_ref, out_ref, mapped_ref, done, *, users, cap, mask):
    fetch = pltpu.make_async_copy(far_ref, mapped_ref, done.at[0])
    fetch.start()
    me = me_ref[0]
    nearest = recv_ref.shape[0] // PLANE // 2
    owners = recv_ref.shape[0]
    rows_dev = mapped_ref.shape[0]
    high = rows_dev // 128
    planes = users // PLANE
    total = planes * high
    most = jnp.zeros((1, 1), F32)
    for g in range(owners // users):
        got = recv_ref[g * users : (g + 1) * users, 0, :]
        to, row, _, _ = decode(me, got, owners, cap, rows_dev)
        key = jnp.where(to >= 0, div_mod(to, PLANE)[0] * high + div_mod(row, 128)[0], -1)
        low = div_mod(row, 128)[1]
        left = [bits(iota((total, cap), 0) == key[u : u + 1, :]) for u in range(users)]
        right = [bits(iota((128, cap), 0) == low[u : u + 1, :]) for u in range(users)]
        seen = dot_nt(jnp.concatenate(left, axis=1), jnp.concatenate(right, axis=1))
        present = bits(seen > 0.0)
        within = dot(present, bits(iota((128, 128), 0) < iota((128, 128), 1)))
        sums = dot(present, jnp.ones((128, 128), BF16)).astype(BF16)
        pi, hi = div_mod(iota((total, total), 0), high)
        pj, hj = div_mod(iota((total, total), 1), high)
        rank = within + dot(bits((pi == pj) & (hj < hi)), sums)
        ranks_ref[g * total : (g + 1) * total, :] = jnp.where(seen > 0.0, rank, -1.0).astype(I32)
        whole = dot(bits(pi == pj), sums)
        plane = div_mod(iota((total, 128), 0), high)[0] + g * planes
        other = jnp.where((plane ^ div_mod(me, PLANE)[0]) < nearest, 0.0, whole)
        most = jnp.maximum(most, jnp.max(jnp.max(other, axis=1, keepdims=True), axis=0, keepdims=True))
    over_ref[...] = jnp.broadcast_to(jnp.where(most > out_ref.shape[0], 1.0, 0.0), over_ref.shape)
    fetch.wait()
    send_set(me, mask, ranks_ref, mapped_ref, out_ref)


def index_kernel(me_ref, recv_ref, ranks_ref, over_ref, index_ref, *outs, masks, cap, rows_dev):
    me = me_ref[0]
    groups, room, users = index_ref.shape
    wide = outs[0].shape[1]
    high = rows_dev // 128
    for g in range(groups):
        got = recv_ref[g * users : (g + 1) * users, 0, :]
        index_ref[g] = index_of(me, got, recv_ref.shape[0], cap, room, rows_dev)
    same = iota((room, wide), 0) == iota((room, wide), 1)
    for mask, out_ref in zip(masks, outs):
        plane = div_mod(me, PLANE)[0] ^ mask
        out_ref[...] = jnp.broadcast_to(over_ref[0:1, 0:1], out_ref.shape)
        ranks = ranks_ref[pl.ds(pl.multiple_of(plane * high, high), high), :]

        def one(j, carry, out_ref=out_ref, plane=plane, ranks=ranks):
            group, loc = div_mod(plane * PLANE + j, users)
            index = index_ref[group]
            column = jnp.sum(jnp.where(iota(index.shape, 1) == loc, index, 0.0), axis=1, keepdims=True).astype(I32)
            found = jnp.zeros((room, 128), I32)
            for h in range(high):
                found = jnp.where(iota((room, 128), 1) + 128 * h == column, ranks[h : h + 1, :], found)
            place = jnp.sum(found.astype(F32), axis=1, keepdims=True)
            out_ref[pl.ds(j, 1), :] = jnp.sum(jnp.where(same, place, 0.0), axis=0, keepdims=True)
            return carry

        lax.fori_loop(0, PLANE, one, 0)


def sets_kernel(me_ref, ranks_ref, mapped_ref, after_ref, order_ref, *outs, masks):
    for mask, out_ref in zip(masks, outs):
        send_set(me_ref[0], mask, ranks_ref, mapped_ref, out_ref)
    order_ref[...] = jnp.zeros(order_ref.shape, F32)


def store_each(one, outs, block_ref):
    def step(i, carry):
        block_ref[...] = one(i)
        for k, out_ref in enumerate(outs):
            @pl.when(i == k)
            def _(out_ref=out_ref):
                out_ref[...] = block_ref[...]
        return carry

    lax.fori_loop(0, len(outs), step, 0)


def near_kernel(me_ref, index_ref, mapped_ref, after_ref, order_ref, *refs, first):
    users = index_ref.shape[2]

    def one(i):
        group, loc = div_mod(me_ref[0] ^ (first + i), users)
        return gather_rows(index_ref[group], mapped_ref, loc)

    store_each(one, refs[:-1], refs[-1])
    order_ref[...] = jnp.zeros(order_ref.shape, F32)


def relay_kernel(me_ref, set_ref, places_ref, after_ref, order_ref, *refs, first):
    many = set_ref.shape[0]
    wide = places_ref.shape[1]
    room = refs[-1].shape[0]
    same = iota((room, wide), 0) == iota((room, wide), 1)
    over = places_ref[PLANE : PLANE + 1, 0:1]

    def one(i):
        j = div_mod(me_ref[0] ^ (first + i), PLANE)[1]
        column = jnp.sum(jnp.where(same, places_ref[pl.ds(j, 1), :], 0.0), axis=1, keepdims=True).astype(I32)
        onehot = bits(iota((room, many), 1) == column)
        got = dot(onehot, set_ref[...])
        return jnp.where(iota(got.shape, 0) == room - 1, over, got).astype(BF16)

    store_each(one, refs[:-1], refs[-1])
    order_ref[...] = jnp.zeros(order_ref.shape, F32)


def meta_kernel(me_ref, recv_ref, after_ref, seed_ref, user_ref, order_ref, *, users, hist, rows_dev, seeds):
    owners, room = seed_ref.shape
    group = pl.multiple_of(div_mod(me_ref[0], users)[0] * users, users)
    meta = recv_ref[pl.ds(group, users), 0, recv_ref.shape[2] - hist :]
    ids, seed = div_mod(meta, seeds)
    owner = jnp.where(meta >= 0, div_mod(ids, rows_dev)[0] ^ me_ref[0], -1)
    pos, _ = positions(owner, owners)
    slot = iota((room, hist), 0)
    shard = iota((owners, hist), 0)
    found = jnp.zeros((2 * owners, room), F32)
    for u in range(users):
        onehot = bits(slot == pos[u : u + 1, :])
        mine = shard == owner[u : u + 1, :]
        both = jnp.concatenate([jnp.where(mine, seed[u : u + 1, :].astype(F32), 0.0), jnp.where(mine, u + 1.0, 0.0)], axis=0)
        found = found + dot_nt(both.astype(BF16), onehot)
    order_ref[...] = jnp.zeros(order_ref.shape, F32)
    seed_ref[...] = found[:owners].astype(I32)
    user_ref[...] = found[owners:].astype(I32)


def route(logits_of, rows_refs, user_ref, summed_ref, logits_ref):
    owners = len(rows_refs)
    lanes = summed_ref.shape[0]
    for s in range(owners):
        logits = logits_of(s)
        if logits_ref is not None:
            logits_ref[s] = logits
        caps = logits.shape[0]
        user = user_ref[s : s + 1, :]
        top = jnp.max(logits, axis=0, keepdims=True)
        raised = jnp.exp(logits - top)
        weights = raised / jnp.sum(raised, axis=0, keepdims=True)
        spread = jnp.concatenate([jnp.where(user == u + 1, weights, 0.0) for u in range(lanes // caps)], axis=0)
        part = dot(spread.astype(BF16), rows_refs[s][...])
        if s == 0:
            summed_ref[...] = part
        else:
            summed_ref[...] += part


def chosen(values, user, caps):
    total = jnp.zeros((caps, user.shape[1]), F32)
    for u in range(values.shape[0] // caps):
        total = jnp.where(user == u + 1, values[u * caps : (u + 1) * caps], total)
    return total


def products(rows_refs, user_ref, summed_ref, sent_ref, caps):
    owners, room = len(rows_refs), rows_refs[0].shape[0]
    summed = summed_ref[...]
    lanes = summed.shape[0]
    high = summed.astype(BF16)
    low = (summed - high.astype(F32)).astype(BF16)
    both = jnp.concatenate([high, low], axis=0)
    for s in range(owners):
        dots = dot_nt(both, rows_refs[s][...])
        dots = dots[:lanes] + dots[lanes:]
        sent_ref[s * caps : (s + 1) * caps, :room] = chosen(dots, user_ref[s : s + 1, :], caps)
    sent_ref[:lanes, room:] = jnp.broadcast_to(
        jnp.sum(summed * summed, axis=1, keepdims=True), (lanes, sent_ref.shape[1] - room)
    )
    if sent_ref.shape[0] > lanes:
        sent_ref[lanes:, room:] = jnp.zeros((sent_ref.shape[0] - lanes, sent_ref.shape[1] - room), F32)


def first_kernel(*refs, owners):
    rows_refs, (seed_ref, user_ref, table_ref, logits_ref, sent_ref, summed_ref, flag_ref) = refs[:owners], refs[owners:]
    caps, seeds = table_ref.shape
    room = rows_refs[0].shape[0]

    def initial(s):
        onehot = jnp.where(iota((seeds, room), 0) == seed_ref[s : s + 1, :], 1.0, 0.0)
        return jnp.dot(table_ref[...], onehot, precision=lax.Precision.HIGHEST, preferred_element_type=F32)

    flags = sum(ref[room - 16 :, :128].astype(F32) for ref in rows_refs[owners // 2 :])[15:]
    flag_ref[...] = jnp.broadcast_to(flags, flag_ref.shape)
    route(initial, rows_refs, user_ref, summed_ref, logits_ref)
    products(rows_refs, user_ref, summed_ref, sent_ref, caps)


def later_kernel(*refs, cols, last, owners, lanes):
    parts, rows_refs, refs = refs[:cols], refs[cols : cols + owners], refs[cols + owners :]
    (user_ref, old_ref), outs = refs[:2], refs[2:]
    room = rows_refs[0].shape[0]
    caps = old_ref.shape[1]
    squares = sum(part[:lanes, room : room + 1] for part in parts)
    scale = squash_scale(squares)

    def updated(s):
        dots = sum(part[s * caps : (s + 1) * caps, :room] for part in parts)
        user = user_ref[s : s + 1, :]
        wide = jnp.broadcast_to(scale, (lanes, room))
        return old_ref[s] + dots * chosen(wide, user, caps)

    if last:
        summed_ref, square_ref = outs
        route(updated, rows_refs, user_ref, summed_ref, None)
        summed = summed_ref[...]
        square_ref[...] = jnp.broadcast_to(jnp.sum(summed * summed, axis=1, keepdims=True), square_ref.shape)
    else:
        logits_ref, sent_ref, summed_ref = outs
        route(updated, rows_refs, user_ref, summed_ref, logits_ref)
        products(rows_refs, user_ref, summed_ref, sent_ref, caps)


def squash_kernel(summed_ref, flag_ref, *refs):
    scale = squash_scale(sum(part[:, :1] for part in refs[:-1]))
    scale = jnp.where(flag_ref[0:1, 0:1] > 0.0, jnp.nan, scale)
    refs[-1][...] = summed_ref[...] * scale


def call(kernel, out_shape, n_in, smem=(), far=(), far_out=False, flops=0, mib=12, **kw):
    ins = [SMEM if i in smem else FAR if i in far else VMEM for i in range(n_in)]
    size = sum(math.prod(leaf.shape) * leaf.dtype.itemsize for leaf in jax.tree.leaves(out_shape))
    return pl.pallas_call(
        kernel,
        out_shape=out_shape,
        in_specs=ins,
        out_specs=jax.tree.map(lambda _: FAR if far_out else VMEM, out_shape),
        compiler_params=pltpu.CompilerParams(vmem_limit_bytes=mib << 20),
        cost_estimate=pl.CostEstimate(flops=flops, bytes_accessed=size, transcendentals=0),
        **kw,
    )


def shifted(x, by):
    cols = lax.axis_size("cols")
    return lax.ppermute(x, "cols", [((i + by) % cols, i) for i in range(cols)])


def all_cols(x):
    return [x] + [shifted(x, by) for by in range(1, lax.axis_size("cols"))]


def owner_ranks(owner, owners):
    tok_count = owner.shape[0]
    span = min(256, tok_count)
    onehot = (owner[:, None] == jnp.arange(owners, dtype=I32)[None, :]).astype(F32)
    blocked = onehot.reshape(tok_count // span, span, owners)
    lower = (iota((span, span), 0) >= iota((span, span), 1)).astype(F32)
    within = jnp.einsum("ij,bjo->bio", lower, blocked)
    totals = within[:, -1, :]
    before = jnp.cumsum(totals, axis=0) - totals
    counts = (within + before[:, None, :]).reshape(tok_count, owners)
    return (jnp.sum(counts * onehot, axis=1) - 1.0).astype(I32)


def any_input(item_ids, lengths, seed_rows, mapped_rows, seed_table, cap):
    users_here, hist = item_ids.shape
    owners = lax.axis_size("users")
    rows_dev, half = mapped_rows.shape
    tok_count = users_here * hist
    flat_ids = item_ids.reshape(tok_count)
    owner = flat_ids // rows_dev
    slot = owner * cap + owner_ranks(owner, owners)
    requests = jnp.zeros((owners * cap,), I32).at[slot].set(flat_ids % rows_dev).reshape(owners, cap)
    asked = lax.all_to_all(requests, "users", split_axis=0, concat_axis=0, tiled=True)
    answers = lax.all_to_all(mapped_rows[asked], "users", split_axis=0, concat_axis=0, tiled=True)
    mapped = answers.reshape(owners * cap, half)[slot].reshape(users_here, hist, half)
    logits = seed_table[seed_rows]
    live = (jnp.arange(hist, dtype=I32)[None, :] < lengths[:, None]).astype(F32)
    for step in range(ITERS):
        weights = (jax.nn.softmax(logits, axis=-1) * live[:, :, None]).astype(BF16)
        summed = jnp.einsum("utk,utd->ukd", weights, mapped, preferred_element_type=F32)
        squares = sum(all_cols(jnp.sum(summed * summed, axis=-1)))
        scale = squash_scale(squares)
        if step + 1 < ITERS:
            dots = jnp.einsum(
                "utd,ukd->utk", mapped, summed, preferred_element_type=F32, precision=lax.Precision.HIGHEST
            )
            logits = logits + sum(all_cols(dots)) * scale[:, None, :]
    return summed * scale[:, :, None]


def map_table(factor, parts):
    rows_dev, width = parts[0].shape
    half = factor.shape[1]
    tiles = 4
    return call(
        functools.partial(map_kernel, cols=len(parts)),
        pltpu.HBM((rows_dev, half), BF16),
        2 + len(parts),
        smem=(0,),
        far=(1, 2),
        far_out=True,
        flops=2 * rows_dev * half * factor.shape[0],
        scratch_shapes=[
            pltpu.VMEM(factor.shape, BF16),
            pltpu.VMEM((tiles, rows_dev // tiles, width), BF16),
            pltpu.VMEM((tiles, rows_dev // tiles, half), BF16),
            pltpu.SemaphoreType.DMA((2 * tiles + 1,)),
        ],
    )(lax.axis_index("cols").reshape(1), factor, *parts)


def plane_masks(owners):
    planes = owners // PLANE
    return list(range(planes // 2, planes))


def on_device(item_ids, lengths, seed_rows, item_table, bilinear, seed_table):
    users, hist = item_ids.shape
    owners = lax.axis_size("users")
    cols = lax.axis_size("cols")
    me = lax.axis_index("users")
    rows_dev = item_table.shape[0]
    half = bilinear.shape[1]
    seeds, caps = seed_table.shape
    tok_count = users * hist
    cap = max(2, (2 * tok_count + owners - 1) // owners)
    room = -(-cap * 15 // 32 // 16) * 16
    pairs = owners * users
    lanes = users * caps
    assert owners % users == 0 and owners & (owners - 1) == 0
    assert users % PLANE == 0 and rows_dev % 128 == 0
    assert hist <= 256 and seeds <= 256 and rows_dev * users <= 65536
    local = lax.rem(me, users)
    group = me - local
    here = me.reshape(1)

    table_parts = all_cols(item_table)
    blocks, dest = call(
        functools.partial(prep_kernel, owners=owners, rows_dev=rows_dev, seeds=seeds, cap=cap),
        (jax.ShapeDtypeStruct((owners, 1, cap + pairs + hist), I32), jax.ShapeDtypeStruct((users, 1), I32)),
        4,
        smem=(0,),
    )(local.reshape(1), item_ids, seed_rows, lengths.reshape(1, users))
    recv = lax.all_to_all(blocks, "users", split_axis=0, concat_axis=0, tiled=True)
    mapped_rows = map_table(bilinear, table_parts)
    counts = recv[:, 0, cap : cap + pairs].reshape(owners // users, users, pairs)
    fits = jnp.max(jnp.sum(counts, axis=1)) < room

    block = jax.ShapeDtypeStruct((room, half), BF16)
    many = -(-PLANE * room * 11 // 15 // 64) * 64
    one_set = jax.ShapeDtypeStruct((many, half), BF16)
    wide = -(-room // 128) * 128
    mark = jax.ShapeDtypeStruct((8, 128), F32)
    groups = owners // users
    planes = owners // PLANE
    high = rows_dev // 128
    scratch = [pltpu.VMEM((room, half), BF16)]
    set_flops = 2 * many * half * rows_dev

    def send(x, mask):
        return lax.ppermute(x, "users", [(i, i ^ mask) for i in range(owners)])

    masks = plane_masks(owners)
    ranks, over, ready, mapped_rows = call(
        functools.partial(rank_kernel, users=users, cap=cap, mask=masks[0]),
        (jax.ShapeDtypeStruct((planes * high, 128), I32), mark, one_set, jax.ShapeDtypeStruct(mapped_rows.shape, BF16)),
        3,
        smem=(0,),
        far=(2,),
        flops=set_flops,
        scratch_shapes=[pltpu.SemaphoreType.DMA((1,))],
    )(here, recv, pltpu.with_memory_space_constraint(mapped_rows, pltpu.HBM))
    sets = {masks[0]: send(ready, masks[0] * PLANE)}

    def make_sets(chosen, after):
        order, *ready = call(
            functools.partial(sets_kernel, masks=chosen),
            [mark] + [one_set] * len(chosen),
            4,
            smem=(0,),
            flops=set_flops * len(chosen),
        )(here, ranks, mapped_rows, after)
        sets.update({mask: send(x, mask * PLANE) for mask, x in zip(chosen, ready)})
        return order

    index, *places = call(
        functools.partial(index_kernel, masks=masks, cap=cap, rows_dev=rows_dev),
        [jax.ShapeDtypeStruct((groups, room, users), F32)] + [jax.ShapeDtypeStruct((8, wide), F32)] * len(masks),
        4,
        smem=(0,),
        flops=set_flops,
    )(here, recv, ranks, over)
    places = [send(x, mask * PLANE) for mask, x in zip(masks, places)]
    rows = [None] * owners

    def near(first, stop, order):
        order, *blocks_out = call(
            functools.partial(near_kernel, first=first),
            [mark] + [block] * (stop - first),
            4,
            smem=(0,),
            flops=2 * (stop - first) * room * half * rows_dev,
            scratch_shapes=scratch,
        )(here, index, mapped_rows, order)
        for i, out in zip(range(first, stop), blocks_out):
            rows[i] = send(out, i) if i else out
        return order

    order = near(PLANE, owners // 2, index)
    order = near(0, PLANE, order)
    where = jax.ShapeDtypeStruct((owners, room), I32)
    seed, user, order = call(
        functools.partial(meta_kernel, users=users, hist=hist, rows_dev=rows_dev, seeds=seeds), (where, where, mark), 3, smem=(0,)
    )(here, recv, order)
    order = make_sets(masks[1:], order)
    for mask, place in zip(masks, places):
        got = sets[mask]
        for first, stop in RELAYS:
            order, *blocks_out = call(
                functools.partial(relay_kernel, first=first),
                [mark] + [block] * (stop - first),
                4,
                smem=(0,),
                flops=2 * (stop - first) * room * half * many,
                scratch_shapes=scratch,
            )(here, got, place, order)
            for i, out in zip(range(first, stop), blocks_out):
                rows[mask * PLANE + i] = send(out, i) if i else out

    logits_shape = jax.ShapeDtypeStruct((owners, caps, room), F32)
    sent_shape = jax.ShapeDtypeStruct((owners * caps, (room // 128 + 1) * 128), F32)
    summed_shape = jax.ShapeDtypeStruct((lanes, half), F32)
    square_shape = jax.ShapeDtypeStruct((lanes, 128), F32)
    step_shapes = (logits_shape, sent_shape, summed_shape)
    kernel = functools.partial(first_kernel, owners=owners)
    logits, sent, _, flag = call(kernel, step_shapes + (mark,), owners + 3)(*rows, seed, user, seed_table.T)
    later = functools.partial(later_kernel, cols=cols, owners=owners, lanes=lanes)
    for _ in range(ITERS - 2):
        kernel = functools.partial(later, last=False)
        logits, sent, _ = call(kernel, step_shapes, cols + owners + 2)(*all_cols(sent), *rows, user, logits)
    kernel = functools.partial(later, last=True)
    summed, square = call(kernel, (summed_shape, square_shape), cols + owners + 2)(*all_cols(sent), *rows, user, logits)
    capsules = call(squash_kernel, summed_shape, cols + 2)(summed, flag, *all_cols(square)).reshape(users, caps, half)
    if owners > users:
        spread = jnp.zeros((owners, caps, half), F32)
        capsules = lax.dynamic_update_slice_in_dim(spread, capsules, group, 0)
    back = lax.all_to_all(capsules, "users", split_axis=0, concat_axis=0, tiled=True)
    if owners > users:
        back = lax.dynamic_slice_in_dim(back, group, users, 0)
    over = jnp.max(jnp.where(jnp.isnan(back[:, 0, 0]), 1, 0))
    if owners > users:
        over = lax.pmax(over, "users")
    fits = fits & (over == 0)
    dealt = back[dest[:, 0]]

    def kept(dealt, *_):
        return dealt

    def full(dealt, item_table, bilinear, seed_table, item_ids, lengths, seed_rows):
        mapped_rows = map_table(bilinear, all_cols(item_table))
        return any_input(item_ids, lengths, seed_rows, mapped_rows, seed_table, cap)

    return lax.cond(fits, kept, full, dealt, item_table, bilinear, seed_table, item_ids, lengths, seed_rows)


def solution(mesh):
    placed = (
        P("users", None),
        P("users"),
        P("users", None),
        P("users", "cols"),
        P(None, "cols"),
        P(),
    )

    return jax.shard_map(on_device, mesh=mesh, in_specs=placed, out_specs=P("users", None, "cols"), check_vma=False)
```

```python
import functools
import math

import jax
import jax.numpy as jnp
from jax import lax
from jax.experimental import pallas as pl
from jax.experimental.pallas import tpu as pltpu
from jax.sharding import PartitionSpec as P


ITERS = 3
PLANE = 4
RELAYS = ((1, 2), (2, 4), (0, 1))
F32, BF16, I32 = jnp.float32, jnp.bfloat16, jnp.int32
NT = (((1,), (1,)), ((), ()))
VMEM = pl.BlockSpec(memory_space=pltpu.VMEM)
SMEM = pl.BlockSpec(memory_space=pltpu.SMEM)
FAR = pl.BlockSpec(memory_space=pltpu.HBM)


def squash_scale(squares):
    return squares / (1.0 + squares) / jnp.sqrt(squares + 1e-06)


def div_mod(value, by):
    if by & (by - 1) == 0:
        return value >> (by.bit_length() - 1), value & (by - 1)
    quotient = lax.div(value, jnp.full(value.shape, by, I32))
    return quotient, value - quotient * by


def iota(shape, dim):
    return lax.broadcasted_iota(I32, shape, dim)


def dot(a, b):
    return jnp.dot(a, b, preferred_element_type=F32)


def dot_nt(a, b, **kw):
    return lax.dot_general(a, b, NT, preferred_element_type=F32, **kw)


def bits(mask):
    return jnp.where(mask, 1.0, 0.0).astype(BF16)


def halves(mask, value):
    low = value & 255
    both = [jnp.where(mask, term.astype(F32), 0.0) for term in (low, value - low)]
    return jnp.concatenate(both, axis=0).astype(BF16)


def positions(owner, owners):
    users, hist = owner.shape
    masks = jnp.concatenate([jnp.where(owner == s, 1.0, 0.0) for s in range(owners)], axis=0).astype(BF16)
    before = bits(iota((hist, hist), 0) < iota((hist, hist), 1))
    within = dot(masks, before)
    totals = dot(masks, jnp.ones((hist, hist), BF16))
    stacked = owners * users
    si, ui = div_mod(iota((stacked, stacked), 0), users)
    sj, uj = div_mod(iota((stacked, stacked), 1), users)
    earlier = dot(bits((si == sj) & (uj < ui)), totals.astype(BF16))
    rank = within + earlier
    pos = jnp.full(owner.shape, -1.0, F32)
    for s in range(owners):
        pos = jnp.where(owner == s, rank[s * users : (s + 1) * users], pos)
    return pos.astype(I32), masks


def prep_kernel(local_ref, ids_ref, seeds_ref, row_ref, blocks_ref, dest_ref, *, owners, rows_dev, seeds, cap):
    users, hist = ids_ref.shape
    row = row_ref[...]
    i, j = iota((users, users), 1), iota((users, users), 0)
    col = jnp.sum(jnp.where(i == j, row.astype(F32), 0.0), axis=1, keepdims=True).astype(I32)
    ahead = (row > col) | ((row == col) & (i < j))
    rank = jnp.sum(jnp.where(ahead, 1.0, 0.0), axis=1, keepdims=True).astype(I32)
    turn = div_mod(rank + local_ref[0], users)[1]
    high, low = div_mod(turn, users // PLANE)
    dest = low * PLANE + high
    dest_ref[...] = dest
    live = iota((users, hist), 1) < col
    packed = jnp.where(live, ids_ref[...] * seeds + seeds_ref[...], -1)
    place = iota((users, hist), 0)
    meta = jnp.full((users, hist), -1, I32)
    for j in range(users):
        meta = jnp.where(place == dest[j : j + 1, :], packed[j : j + 1, :], meta)
    ids = div_mod(meta, seeds)[0]
    owner, row_in = div_mod(ids, rows_dev)
    owner = jnp.where(meta >= 0, owner, -1)
    pos, masks = positions(owner, owners)
    lists = jnp.zeros((2 * owners, cap), F32)
    slot = iota((cap, hist), 0)
    shard = iota((owners, hist), 0)
    for v in range(users):
        onehot = bits(slot == pos[v : v + 1, :])
        mine = shard == owner[v : v + 1, :]
        lists = lists + dot_nt(halves(mine, row_in[v : v + 1, :] + v * rows_dev), onehot)
    lists = lists[:owners] + lists[owners:]
    counts = dot_nt(jnp.ones((8, hist), BF16), masks)
    pairs = owners * users
    blocks_ref[:, 0, :cap] = lists.astype(I32)
    blocks_ref[:, 0, cap : cap + pairs] = jnp.broadcast_to(counts[:1].astype(I32), (owners, pairs))
    for group in range(owners // users):
        blocks_ref[group * users : (group + 1) * users, 0, cap + pairs :] = meta


def map_kernel(*refs, cols):
    at_ref, factor_ref, own_ref, others = refs[0], refs[1], refs[2], refs[3 : 2 + cols]
    out_ref, factor, own, block, done = refs[2 + cols :]
    rows, width = own_ref.shape
    tall = own.shape[1]
    tiles = rows // tall

    def fetch(i):
        return pltpu.make_async_copy(own_ref.at[pl.ds(i * tall, tall)], own.at[i], done.at[i])

    def store(i):
        return pltpu.make_async_copy(block.at[i], out_ref.at[pl.ds(i * tall, tall)], done.at[tiles + i])

    whole = pltpu.make_async_copy(factor_ref, factor, done.at[2 * tiles])
    whole.start()
    for i in range(tiles):
        fetch(i).start()
    whole.wait()
    for i in range(tiles):
        fetch(i).wait()
        total = None
        for by in range(cols):
            part = own[i] if by == 0 else others[by - 1][i * tall : (i + 1) * tall, :]
            at = pl.multiple_of(lax.rem(at_ref[0] + by, cols) * width, width)
            term = dot(part, factor[pl.ds(at, width), :])
            total = term if total is None else total + term
        block[i] = total.astype(BF16)
        store(i).start()
    for i in range(tiles):
        store(i).wait()


def gather_rows(index, mapped_ref, loc):
    column = jnp.sum(jnp.where(iota(index.shape, 1) == loc, index, 0.0), axis=1, keepdims=True)
    onehot = bits(iota((index.shape[0], mapped_ref.shape[0]), 1) == column.astype(I32))
    return dot(onehot, mapped_ref[...]).astype(BF16)


def decode(me, got, owners, cap, rows_dev):
    users = got.shape[0]
    pairs = owners * users
    lists, counts = got[:, :cap], got[:, cap : cap + pairs].astype(F32).astype(BF16)
    s, w = div_mod(iota((pairs, 128), 0), users)
    lane = iota((pairs, 128), 1)
    here = s == me
    count = dot(counts, bits(here & (w == lane)))
    start = dot(counts, bits(here & (w < lane)))
    valid = iota((users, cap), 1) < start[:, users : users + 1].astype(I32)
    to, row = div_mod(lists, rows_dev)
    return jnp.where(valid, to, -1), row, count, start


def index_of(me, got, owners, cap, room, rows_dev):
    users = got.shape[0]
    to, row, count, start = decode(me, got, owners, cap, rows_dev)
    earlier = bits(iota((users, users), 1) < iota((users, users), 0))
    delta = (dot(earlier, count.astype(BF16)) - start).astype(I32)
    pos = iota((users, cap), 1)
    for w in range(users):
        pos = pos + jnp.where(to == w, delta[:, w : w + 1], 0)
    pos = jnp.where(to >= 0, pos, -1)
    slot = iota((room, cap), 0)
    shard = iota((users, cap), 0)
    index = jnp.zeros((room, 2 * users), F32)
    for u in range(users):
        onehot = bits(slot == pos[u : u + 1, :])
        mine = shard == to[u : u + 1, :]
        index = index + dot_nt(onehot, halves(mine, row[u : u + 1, :]))
    return index[:, :users] + index[:, users:]


def send_set(me, mask, ranks_ref, mapped_ref, out_ref):
    high = mapped_ref.shape[0] // 128
    many = out_ref.shape[0]
    tall = many // 4 if many % 64 == 0 else many
    plane = div_mod(me, PLANE)[0] ^ mask
    ranks = ranks_ref[pl.ds(pl.multiple_of(plane * high, high), high), :]

    def one(t, carry):
        slot = iota((tall, 128), 0) + t * tall
        onehot = [bits(slot == ranks[h : h + 1, :]) for h in range(high)]
        here = pl.ds(pl.multiple_of(t * tall, tall), tall)
        out_ref[here, :] = dot(jnp.concatenate(onehot, axis=1), mapped_ref[...]).astype(BF16)
        return carry

    lax.fori_loop(0, many // tall, one, 0, unroll=True)


def rank_kernel(me_ref, recv_ref, far_ref, ranks_ref, over_ref, out_ref, mapped_ref, done, *, users, cap, mask):
    fetch = pltpu.make_async_copy(far_ref, mapped_ref, done.at[0])
    fetch.start()
    me = me_ref[0]
    nearest = recv_ref.shape[0] // PLANE // 2
    owners = recv_ref.shape[0]
    rows_dev = mapped_ref.shape[0]
    high = rows_dev // 128
    planes = users // PLANE
    total = planes * high
    most = jnp.zeros((1, 1), F32)
    for g in range(owners // users):
        got = recv_ref[g * users : (g + 1) * users, 0, :]
        to, row, _, _ = decode(me, got, owners, cap, rows_dev)
        key = jnp.where(to >= 0, div_mod(to, PLANE)[0] * high + div_mod(row, 128)[0], -1)
        low = div_mod(row, 128)[1]
        left = [bits(iota((total, cap), 0) == key[u : u + 1, :]) for u in range(users)]
        right = [bits(iota((128, cap), 0) == low[u : u + 1, :]) for u in range(users)]
        seen = dot_nt(jnp.concatenate(left, axis=1), jnp.concatenate(right, axis=1))
        present = bits(seen > 0.0)
        within = dot(present, bits(iota((128, 128), 0) < iota((128, 128), 1)))
        sums = dot(present, jnp.ones((128, 128), BF16)).astype(BF16)
        pi, hi = div_mod(iota((total, total), 0), high)
        pj, hj = div_mod(iota((total, total), 1), high)
        rank = within + dot(bits((pi == pj) & (hj < hi)), sums)
        ranks_ref[g * total : (g + 1) * total, :] = jnp.where(seen > 0.0, rank, -1.0).astype(I32)
        whole = dot(bits(pi == pj), sums)
        plane = div_mod(iota((total, 128), 0), high)[0] + g * planes
        other = jnp.where((plane ^ div_mod(me, PLANE)[0]) < nearest, 0.0, whole)
        most = jnp.maximum(most, jnp.max(jnp.max(other, axis=1, keepdims=True), axis=0, keepdims=True))
    over_ref[...] = jnp.broadcast_to(jnp.where(most > out_ref.shape[0], 1.0, 0.0), over_ref.shape)
    fetch.wait()
    send_set(me, mask, ranks_ref, mapped_ref, out_ref)


def index_kernel(me_ref, recv_ref, over_ref, index_ref, *, cap, rows_dev):
    groups, room, users = index_ref.shape
    for g in range(groups):
        got = recv_ref[g * users : (g + 1) * users, 0, :]
        index_ref[g] = index_of(me_ref[0], got, recv_ref.shape[0], cap, room, rows_dev)


def places_kernel(me_ref, index_ref, ranks_ref, over_ref, after_ref, order_ref, *outs, masks, rows_dev):
    me = me_ref[0]
    _, room, users = index_ref.shape
    wide = outs[0].shape[1]
    high = rows_dev // 128
    order_ref[...] = jnp.zeros(order_ref.shape, F32)
    same = iota((room, wide), 0) == iota((room, wide), 1)
    for mask, out_ref in zip(masks, outs):
        plane = div_mod(me, PLANE)[0] ^ mask
        out_ref[...] = jnp.broadcast_to(over_ref[0:1, 0:1], out_ref.shape)
        ranks = ranks_ref[pl.ds(pl.multiple_of(plane * high, high), high), :]

        def one(j, carry, out_ref=out_ref, plane=plane, ranks=ranks):
            group, loc = div_mod(plane * PLANE + j, users)
            index = index_ref[group]
            column = jnp.sum(jnp.where(iota(index.shape, 1) == loc, index, 0.0), axis=1, keepdims=True).astype(I32)
            found = jnp.zeros((room, 128), I32)
            for h in range(high):
                found = jnp.where(iota((room, 128), 1) + 128 * h == column, ranks[h : h + 1, :], found)
            place = jnp.sum(found.astype(F32), axis=1, keepdims=True)
            out_ref[pl.ds(j, 1), :] = jnp.sum(jnp.where(same, place, 0.0), axis=0, keepdims=True)
            return carry

        lax.fori_loop(0, PLANE, one, 0)


def sets_kernel(me_ref, ranks_ref, mapped_ref, after_ref, order_ref, *outs, masks):
    for mask, out_ref in zip(masks, outs):
        send_set(me_ref[0], mask, ranks_ref, mapped_ref, out_ref)
    order_ref[...] = jnp.zeros(order_ref.shape, F32)


def store_each(one, outs, block_ref):
    def step(i, carry):
        block_ref[...] = one(i)
        for k, out_ref in enumerate(outs):
            @pl.when(i == k)
            def _(out_ref=out_ref):
                out_ref[...] = block_ref[...]
        return carry

    lax.fori_loop(0, len(outs), step, 0)


def near_kernel(me_ref, index_ref, mapped_ref, after_ref, order_ref, *refs, first):
    users = index_ref.shape[2]

    def one(i):
        group, loc = div_mod(me_ref[0] ^ (first + i), users)
        return gather_rows(index_ref[group], mapped_ref, loc)

    store_each(one, refs[:-1], refs[-1])
    order_ref[...] = jnp.zeros(order_ref.shape, F32)


def relay_kernel(me_ref, set_ref, places_ref, after_ref, order_ref, *refs, first):
    many = set_ref.shape[0]
    wide = places_ref.shape[1]
    room = refs[-1].shape[0]
    same = iota((room, wide), 0) == iota((room, wide), 1)
    over = places_ref[PLANE : PLANE + 1, 0:1]

    def one(i):
        j = div_mod(me_ref[0] ^ (first + i), PLANE)[1]
        column = jnp.sum(jnp.where(same, places_ref[pl.ds(j, 1), :], 0.0), axis=1, keepdims=True).astype(I32)
        onehot = bits(iota((room, many), 1) == column)
        got = dot(onehot, set_ref[...])
        return jnp.where(iota(got.shape, 0) == room - 1, over, got).astype(BF16)

    store_each(one, refs[:-1], refs[-1])
    order_ref[...] = jnp.zeros(order_ref.shape, F32)


def meta_kernel(me_ref, recv_ref, after_ref, seed_ref, user_ref, order_ref, *, users, hist, rows_dev, seeds):
    owners, room = seed_ref.shape
    group = pl.multiple_of(div_mod(me_ref[0], users)[0] * users, users)
    meta = recv_ref[pl.ds(group, users), 0, recv_ref.shape[2] - hist :]
    ids, seed = div_mod(meta, seeds)
    owner = jnp.where(meta >= 0, div_mod(ids, rows_dev)[0] ^ me_ref[0], -1)
    pos, _ = positions(owner, owners)
    slot = iota((room, hist), 0)
    shard = iota((owners, hist), 0)
    found = jnp.zeros((2 * owners, room), F32)
    for u in range(users):
        onehot = bits(slot == pos[u : u + 1, :])
        mine = shard == owner[u : u + 1, :]
        both = jnp.concatenate([jnp.where(mine, seed[u : u + 1, :].astype(F32), 0.0), jnp.where(mine, u + 1.0, 0.0)], axis=0)
        found = found + dot_nt(both.astype(BF16), onehot)
    order_ref[...] = jnp.zeros(order_ref.shape, F32)
    seed_ref[...] = found[:owners].astype(I32)
    user_ref[...] = found[owners:].astype(I32)


def route(logits_of, rows_refs, user_ref, summed_ref, logits_ref, blocks=None, more=False):
    lanes = summed_ref.shape[0]
    for s in blocks or range(len(rows_refs)):
        logits = logits_of(s)
        if logits_ref is not None:
            logits_ref[s] = logits
        caps = logits.shape[0]
        user = user_ref[s : s + 1, :]
        top = jnp.max(logits, axis=0, keepdims=True)
        raised = jnp.exp(logits - top)
        weights = raised / jnp.sum(raised, axis=0, keepdims=True)
        spread = jnp.concatenate([jnp.where(user == u + 1, weights, 0.0) for u in range(lanes // caps)], axis=0)
        part = dot(spread.astype(BF16), rows_refs[s][...])
        if s == 0 and not more:
            summed_ref[...] = part
        else:
            summed_ref[...] += part


def chosen(values, user, caps):
    total = jnp.zeros((caps, user.shape[1]), F32)
    for u in range(values.shape[0] // caps):
        total = jnp.where(user == u + 1, values[u * caps : (u + 1) * caps], total)
    return total


def products(rows_refs, user_ref, summed_ref, sent_ref, caps):
    owners, room = len(rows_refs), rows_refs[0].shape[0]
    summed = summed_ref[...]
    lanes = summed.shape[0]
    high = summed.astype(BF16)
    low = (summed - high.astype(F32)).astype(BF16)
    both = jnp.concatenate([high, low], axis=0)
    for s in range(owners):
        dots = dot_nt(both, rows_refs[s][...])
        dots = dots[:lanes] + dots[lanes:]
        sent_ref[s * caps : (s + 1) * caps, :room] = chosen(dots, user_ref[s : s + 1, :], caps)
    sent_ref[:lanes, room:] = jnp.broadcast_to(
        jnp.sum(summed * summed, axis=1, keepdims=True), (lanes, sent_ref.shape[1] - room)
    )
    if sent_ref.shape[0] > lanes:
        sent_ref[lanes:, room:] = jnp.zeros((sent_ref.shape[0] - lanes, sent_ref.shape[1] - room), F32)


def flags_of(rows_refs):
    room = rows_refs[0].shape[0]
    return sum(ref[room - 16 :, :128].astype(F32) for ref in rows_refs)[15:]


def early_kernel(*refs, blocks, first_flag):
    rows_refs, (seed_ref, user_ref, table_ref, logits_ref, summed_ref, flag_ref) = refs[:blocks], refs[blocks:]
    _, seeds = table_ref.shape
    owners, room = seed_ref.shape
    for s in range(owners):
        onehot = jnp.where(iota((seeds, room), 0) == seed_ref[s : s + 1, :], 1.0, 0.0)
        logits_ref[s] = jnp.dot(table_ref[...], onehot, precision=lax.Precision.HIGHEST, preferred_element_type=F32)
    flag = jnp.zeros((1, 128), F32)
    if first_flag < blocks:
        flag = flags_of(rows_refs[first_flag:])
    flag_ref[...] = jnp.broadcast_to(flag, flag_ref.shape)
    route(lambda s: logits_ref[s], rows_refs, user_ref, summed_ref, None)


def first_kernel(*refs, owners):
    rows_refs, (user_ref, logits_ref, part_ref, early_ref, sent_ref, summed_ref, flag_ref) = refs[:owners], refs[owners:]
    caps = logits_ref.shape[1]
    blocks = range(owners - PLANE, owners)
    flag_ref[...] = early_ref[...] + jnp.broadcast_to(flags_of(rows_refs[owners - PLANE :]), flag_ref.shape)
    summed_ref[...] = part_ref[...]
    route(lambda s: logits_ref[s], rows_refs, user_ref, summed_ref, None, blocks, True)
    products(rows_refs, user_ref, summed_ref, sent_ref, caps)


def later_kernel(*refs, cols, last, owners, lanes):
    parts, rows_refs, refs = refs[:cols], refs[cols : cols + owners], refs[cols + owners :]
    (user_ref, old_ref), outs = refs[:2], refs[2:]
    room = rows_refs[0].shape[0]
    caps = old_ref.shape[1]
    squares = sum(part[:lanes, room : room + 1] for part in parts)
    scale = squash_scale(squares)

    def updated(s):
        dots = sum(part[s * caps : (s + 1) * caps, :room] for part in parts)
        user = user_ref[s : s + 1, :]
        wide = jnp.broadcast_to(scale, (lanes, room))
        return old_ref[s] + dots * chosen(wide, user, caps)

    if last:
        summed_ref, square_ref = outs
        route(updated, rows_refs, user_ref, summed_ref, None)
        summed = summed_ref[...]
        square_ref[...] = jnp.broadcast_to(jnp.sum(summed * summed, axis=1, keepdims=True), square_ref.shape)
    else:
        logits_ref, sent_ref, summed_ref = outs
        route(updated, rows_refs, user_ref, summed_ref, logits_ref)
        products(rows_refs, user_ref, summed_ref, sent_ref, caps)


def squash_kernel(summed_ref, flag_ref, *refs):
    scale = squash_scale(sum(part[:, :1] for part in refs[:-1]))
    scale = jnp.where(flag_ref[0:1, 0:1] > 0.0, jnp.nan, scale)
    refs[-1][...] = (summed_ref[...] * scale).astype(BF16)


def call(kernel, out_shape, n_in, smem=(), far=(), far_out=False, flops=0, mib=12, **kw):
    ins = [SMEM if i in smem else FAR if i in far else VMEM for i in range(n_in)]
    size = sum(math.prod(leaf.shape) * leaf.dtype.itemsize for leaf in jax.tree.leaves(out_shape))
    return pl.pallas_call(
        kernel,
        out_shape=out_shape,
        in_specs=ins,
        out_specs=jax.tree.map(lambda _: FAR if far_out else VMEM, out_shape),
        compiler_params=pltpu.CompilerParams(vmem_limit_bytes=mib << 20),
        cost_estimate=pl.CostEstimate(flops=flops, bytes_accessed=size, transcendentals=0),
        **kw,
    )


def shifted(x, by):
    cols = lax.axis_size("cols")
    return lax.ppermute(x, "cols", [((i + by) % cols, i) for i in range(cols)])


def all_cols(x):
    return [x] + [shifted(x, by) for by in range(1, lax.axis_size("cols"))]


def owner_ranks(owner, owners):
    tok_count = owner.shape[0]
    span = min(256, tok_count)
    onehot = (owner[:, None] == jnp.arange(owners, dtype=I32)[None, :]).astype(F32)
    blocked = onehot.reshape(tok_count // span, span, owners)
    lower = (iota((span, span), 0) >= iota((span, span), 1)).astype(F32)
    within = jnp.einsum("ij,bjo->bio", lower, blocked)
    totals = within[:, -1, :]
    before = jnp.cumsum(totals, axis=0) - totals
    counts = (within + before[:, None, :]).reshape(tok_count, owners)
    return (jnp.sum(counts * onehot, axis=1) - 1.0).astype(I32)


def any_input(item_ids, lengths, seed_rows, mapped_rows, seed_table, cap):
    users_here, hist = item_ids.shape
    owners = lax.axis_size("users")
    rows_dev, half = mapped_rows.shape
    tok_count = users_here * hist
    flat_ids = item_ids.reshape(tok_count)
    owner = flat_ids // rows_dev
    slot = owner * cap + owner_ranks(owner, owners)
    requests = jnp.zeros((owners * cap,), I32).at[slot].set(flat_ids % rows_dev).reshape(owners, cap)
    asked = lax.all_to_all(requests, "users", split_axis=0, concat_axis=0, tiled=True)
    answers = lax.all_to_all(mapped_rows[asked], "users", split_axis=0, concat_axis=0, tiled=True)
    mapped = answers.reshape(owners * cap, half)[slot].reshape(users_here, hist, half)
    logits = seed_table[seed_rows]
    live = (jnp.arange(hist, dtype=I32)[None, :] < lengths[:, None]).astype(F32)
    for step in range(ITERS):
        weights = (jax.nn.softmax(logits, axis=-1) * live[:, :, None]).astype(BF16)
        summed = jnp.einsum("utk,utd->ukd", weights, mapped, preferred_element_type=F32)
        squares = sum(all_cols(jnp.sum(summed * summed, axis=-1)))
        scale = squash_scale(squares)
        if step + 1 < ITERS:
            dots = jnp.einsum(
                "utd,ukd->utk", mapped, summed, preferred_element_type=F32, precision=lax.Precision.HIGHEST
            )
            logits = logits + sum(all_cols(dots)) * scale[:, None, :]
    return summed * scale[:, :, None]


def map_table(factor, parts):
    rows_dev, width = parts[0].shape
    half = factor.shape[1]
    tiles = 4
    return call(
        functools.partial(map_kernel, cols=len(parts)),
        pltpu.HBM((rows_dev, half), BF16),
        2 + len(parts),
        smem=(0,),
        far=(1, 2),
        far_out=True,
        flops=2 * rows_dev * half * factor.shape[0],
        scratch_shapes=[
            pltpu.VMEM(factor.shape, BF16),
            pltpu.VMEM((tiles, rows_dev // tiles, width), BF16),
            pltpu.VMEM((tiles, rows_dev // tiles, half), BF16),
            pltpu.SemaphoreType.DMA((2 * tiles + 1,)),
        ],
    )(lax.axis_index("cols").reshape(1), factor, *parts)


def plane_masks(owners):
    planes = owners // PLANE
    return list(range(planes // 2, planes))


def on_device(item_ids, lengths, seed_rows, item_table, bilinear, seed_table):
    users, hist = item_ids.shape
    owners = lax.axis_size("users")
    cols = lax.axis_size("cols")
    me = lax.axis_index("users")
    rows_dev = item_table.shape[0]
    half = bilinear.shape[1]
    seeds, caps = seed_table.shape
    tok_count = users * hist
    cap = max(2, (2 * tok_count + owners - 1) // owners)
    room = -(-cap * 15 // 32 // 16) * 16
    pairs = owners * users
    lanes = users * caps
    assert owners % users == 0 and owners & (owners - 1) == 0
    assert users % PLANE == 0 and rows_dev % 128 == 0
    assert hist <= 256 and seeds <= 256 and rows_dev * users <= 65536
    local = lax.rem(me, users)
    group = me - local
    here = me.reshape(1)

    table_parts = all_cols(item_table)
    blocks, dest = call(
        functools.partial(prep_kernel, owners=owners, rows_dev=rows_dev, seeds=seeds, cap=cap),
        (jax.ShapeDtypeStruct((owners, 1, cap + pairs + hist), I32), jax.ShapeDtypeStruct((users, 1), I32)),
        4,
        smem=(0,),
    )(local.reshape(1), item_ids, seed_rows, lengths.reshape(1, users))
    recv = lax.all_to_all(blocks, "users", split_axis=0, concat_axis=0, tiled=True)
    mapped_rows = map_table(bilinear, table_parts)
    counts = recv[:, 0, cap : cap + pairs].reshape(owners // users, users, pairs)
    fits = jnp.max(jnp.sum(counts, axis=1)) < room

    block = jax.ShapeDtypeStruct((room, half), BF16)
    many = -(-PLANE * room * 11 // 15 // 64) * 64
    one_set = jax.ShapeDtypeStruct((many, half), BF16)
    wide = -(-room // 128) * 128
    mark = jax.ShapeDtypeStruct((8, 128), F32)
    groups = owners // users
    planes = owners // PLANE
    high = rows_dev // 128
    scratch = [pltpu.VMEM((room, half), BF16)]
    set_flops = 2 * many * half * rows_dev

    def send(x, mask):
        return lax.ppermute(x, "users", [(i, i ^ mask) for i in range(owners)])

    masks = plane_masks(owners)
    ranks, over, ready, mapped_rows = call(
        functools.partial(rank_kernel, users=users, cap=cap, mask=masks[0]),
        (jax.ShapeDtypeStruct((planes * high, 128), I32), mark, one_set, jax.ShapeDtypeStruct(mapped_rows.shape, BF16)),
        3,
        smem=(0,),
        far=(2,),
        flops=set_flops,
        scratch_shapes=[pltpu.SemaphoreType.DMA((1,))],
    )(here, recv, pltpu.with_memory_space_constraint(mapped_rows, pltpu.HBM))
    sets = {masks[0]: send(ready, masks[0] * PLANE)}

    def make_sets(chosen, after):
        order, *ready = call(
            functools.partial(sets_kernel, masks=chosen),
            [mark] + [one_set] * len(chosen),
            4,
            smem=(0,),
            flops=set_flops * len(chosen),
        )(here, ranks, mapped_rows, after)
        sets.update({mask: send(x, mask * PLANE) for mask, x in zip(chosen, ready)})
        return order

    index = call(
        functools.partial(index_kernel, cap=cap, rows_dev=rows_dev),
        jax.ShapeDtypeStruct((groups, room, users), F32),
        3,
        smem=(0,),
        flops=set_flops,
    )(here, recv, over)
    rows = [None] * owners

    def near(first, stop, order):
        order, *blocks_out = call(
            functools.partial(near_kernel, first=first),
            [mark] + [block] * (stop - first),
            4,
            smem=(0,),
            flops=2 * (stop - first) * room * half * rows_dev,
            scratch_shapes=scratch,
        )(here, index, mapped_rows, order)
        for i, out in zip(range(first, stop), blocks_out):
            rows[i] = send(out, i) if i else out
        return order

    order = near(PLANE, owners // 2, index)
    order, *places = call(
        functools.partial(places_kernel, masks=masks, rows_dev=rows_dev),
        [mark] + [jax.ShapeDtypeStruct((8, wide), F32)] * len(masks),
        5,
        smem=(0,),
        flops=set_flops,
    )(here, index, ranks, over, order)
    places = [send(x, mask * PLANE) for mask, x in zip(masks, places)]
    order = near(0, PLANE, order)
    where = jax.ShapeDtypeStruct((owners, room), I32)
    seed, user, order = call(
        functools.partial(meta_kernel, users=users, hist=hist, rows_dev=rows_dev, seeds=seeds), (where, where, mark), 3, smem=(0,)
    )(here, recv, order)
    order = make_sets(masks[1:], order)
    for mask, place in zip(masks, places):
        got = sets[mask]
        for first, stop in RELAYS:
            order, *blocks_out = call(
                functools.partial(relay_kernel, first=first),
                [mark] + [block] * (stop - first),
                4,
                smem=(0,),
                flops=2 * (stop - first) * room * half * many,
                scratch_shapes=scratch,
            )(here, got, place, order)
            for i, out in zip(range(first, stop), blocks_out):
                rows[mask * PLANE + i] = send(out, i) if i else out

    logits_shape = jax.ShapeDtypeStruct((owners, caps, room), F32)
    sent_shape = jax.ShapeDtypeStruct((owners * caps, (room // 128 + 1) * 128), F32)
    summed_shape = jax.ShapeDtypeStruct((lanes, half), F32)
    square_shape = jax.ShapeDtypeStruct((lanes, 128), F32)
    step_shapes = (logits_shape, sent_shape, summed_shape)
    ready = owners - PLANE
    kernel = functools.partial(early_kernel, blocks=ready, first_flag=owners // 2)
    logits, part, flag = call(kernel, (logits_shape, summed_shape, mark), ready + 3)(*rows[:ready], seed, user, seed_table.T)
    kernel = functools.partial(first_kernel, owners=owners)
    sent, _, flag = call(kernel, (sent_shape, summed_shape, mark), owners + 4)(*rows, user, logits, part, flag)
    later = functools.partial(later_kernel, cols=cols, owners=owners, lanes=lanes)
    for _ in range(ITERS - 2):
        kernel = functools.partial(later, last=False)
        logits, sent, _ = call(kernel, step_shapes, cols + owners + 2)(*all_cols(sent), *rows, user, logits)
    kernel = functools.partial(later, last=True)
    summed, square = call(kernel, (summed_shape, square_shape), cols + owners + 2)(*all_cols(sent), *rows, user, logits)
    sent_back = jax.ShapeDtypeStruct((lanes, half), BF16)
    capsules = call(squash_kernel, sent_back, cols + 2)(summed, flag, *all_cols(square)).reshape(users, caps, half)
    if owners > users:
        spread = jnp.zeros((owners, caps, half), BF16)
        capsules = lax.dynamic_update_slice_in_dim(spread, capsules, group, 0)
    back = lax.all_to_all(capsules, "users", split_axis=0, concat_axis=0, tiled=True)
    if owners > users:
        back = lax.dynamic_slice_in_dim(back, group, users, 0)
    over = jnp.max(jnp.where(jnp.isnan(back[:, 0, 0]), 1, 0))
    if owners > users:
        over = lax.pmax(over, "users")
    fits = fits & (over == 0)
    dealt = back[dest[:, 0]].astype(F32)

    def kept(dealt, *_):
        return dealt

    def full(dealt, item_table, bilinear, seed_table, item_ids, lengths, seed_rows):
        mapped_rows = map_table(bilinear, all_cols(item_table))
        return any_input(item_ids, lengths, seed_rows, mapped_rows, seed_table, cap)

    return lax.cond(fits, kept, full, dealt, item_table, bilinear, seed_table, item_ids, lengths, seed_rows)


def solution(mesh):
    placed = (
        P("users", None),
        P("users"),
        P("users", None),
        P("users", "cols"),
        P(None, "cols"),
        P(),
    )

    return jax.shard_map(on_device, mesh=mesh, in_specs=placed, out_specs=P("users", None, "cols"), check_vma=False)
```
